32 devices in a mesh: img: 2 (over core), band: 4 (over z), pw: 4 (over y, x).
Axes of the slice: x: 2, y: 2, z: 4, core: 2. Of those that a mesh axis runs over, the one named last changes fastest.
Arguments:
- coefficients: bfloat16 [2, 1024, 32, 2048], P('img', None, ('band', 'pw')), may hold values from -6 to 6
- rotation: bfloat16 [2, 1024, 256], P('img'), may hold values from -0.1875 to 0.1875
- positions: int32 [2, 3, 256], P('img'), may hold values from 0 to 63, as said below
- start_pos: int32 [3, 256], replicated, may hold values from 0 to 63, as said below
- end_pos: int32 [3, 256], replicated, may hold values from 0 to 63, as said below
- species: int32 [256], replicated, may hold values from 0 to 3
- depth: float32 [4], replicated, may hold values from 0.5 to 3
Outputs:
- correction: bfloat16 [2, 256, 32, 2048], P('img', None, ('band', 'pw'))
- ritz_values: float32 [2, 256], P('img')
- band_force: float32 [2, 3, 256], P('img')
- along_force: float32 [2], P('img')
The draws below stay inside these ranges and needn't reach their ends.
Inputs may be any that keep to these rules, and one draw needn't show every extreme that they name: `positions`: grid index of each atom's centre along each dimension. `start_pos`: grid index of each atom's centre along each dimension. `end_pos`: grid index of each atom's centre along each dimension.
All inputs are finite; a program needn't handle non-finite values.
Results may differ from the reference program's by a relative error of at most 0.012.
The reference program's roundings to bfloat16 on the way count: a program that leaves them out, or rounds other values in their place, can miss the bound.
Values may be sent and summed in bfloat16 or wider, within the bound.
A program may use at most 128 MiB of HBM per device.

```python
import math
import jax
import jax.numpy as jnp
from jax import lax

G = 64
W = 32
BANDS = 1024
BLOCK = 256
ATOMS = 256
SPECIES = 4
IMAGES = 2
NPW = 32768


def common_base(key):
    return jax.random.randint(jax.random.fold_in(key, 11), (3, ATOMS), 0, G)


def displaced(key, salt_value, shape_full):
    return jax.random.randint(jax.random.fold_in(key, salt_value), shape_full, -2, 3)


def draw_positions(key, part):
    base_grid = common_base(key)
    return jnp.mod(base_grid[None] + displaced(key, 12, (IMAGES, 3, ATOMS)), G).astype(jnp.int32)


def draw_start_pos(key, part):
    base_grid = common_base(key)
    return jnp.mod(base_grid + displaced(key, 13, (3, ATOMS)), G).astype(jnp.int32)


def draw_end_pos(key, part):
    base_grid = common_base(key)
    return jnp.mod(base_grid + displaced(key, 14, (3, ATOMS)), G).astype(jnp.int32)


def with_ends(values, stream_key, least, high):
    index_at = [jax.random.randint(jax.random.fold_in(stream_key, axis), (), 0, length) for axis, length in enumerate(values.shape)]
    main_axis = values.shape.index(max(values.shape))
    next_to = index_at[:main_axis] + [(index_at[main_axis] + 1) % values.shape[main_axis]] + index_at[main_axis + 1:]
    return values.at[tuple(index_at)].set(least).at[tuple(next_to)].set(high)


def levels(own_key, shape, pieces, smallest, largest):
    level = 1.0
    for axis_at, shards_of in pieces:
        steps = jax.random.uniform(jax.random.fold_in(jax.random.fold_in(own_key, 6), axis_at), (shards_of,), jnp.float32, smallest / len(pieces), largest / len(pieces))
        level = level * jnp.repeat(jnp.exp(steps), shape[axis_at] // shards_of).reshape((-1,) + (1,) * (len(shape) - 1 - axis_at))
    return level


def normal_values(own_key, shape, scale, reach, pieces=(), held_as=jnp.bfloat16):
    drawn = jax.random.normal(own_key, shape, jnp.float32) * scale
    if len(pieces) > 0:
        drawn = levels(own_key, shape, pieces, -0.22, 0.18) * drawn
    return jnp.clip(drawn, min=-reach, max=reach).astype(held_as)


def setup_inputs(seed: int = 0) -> dict:
    splits = jax.random.split(jax.random.key(seed), 8)
    return {
        "coefficients": normal_values(splits[0], (IMAGES, BANDS, W, W * 2 * W), 1.0, 6.0, ((0, 2), (2, 16))),
        "rotation": normal_values(splits[1], (IMAGES, BANDS, BLOCK), BANDS ** -0.5, 0.1875, ((0, 2),)),
        "positions": draw_positions(jax.random.fold_in(splits[7], 71), 0),
        "start_pos": draw_start_pos(jax.random.fold_in(splits[7], 71), 0),
        "end_pos": draw_end_pos(jax.random.fold_in(splits[7], 71), 0),
        "species": with_ends(jax.random.randint(splits[5], (ATOMS,), 0, SPECIES), jax.random.fold_in(splits[5], 1), 0, SPECIES - 1).astype(jnp.int32),
        "depth": jnp.clip(jnp.exp(jax.random.uniform(splits[6], (SPECIES,), jnp.float32, math.log(0.5), math.log(3.0))), 0.5, 3.0),
    }


kinetic_scale = 0.01
sigma_cells = 3.0
spring_constant = 2.0
epsilon = 1e-06
highest = lax.Precision.HIGHEST

def product(pattern, left_op, right_op):
    return jnp.einsum(pattern, left_op.astype(jnp.float32), right_op.astype(jnp.float32), precision=highest)

def phases(box_order, box_size, grid_size):
    wavenum = box_order.astype(jnp.int32) - box_size // 2
    grid_cells = jnp.arange(grid_size, dtype=jnp.int32)
    turn_count = jnp.mod(wavenum[:, None] * grid_cells[None, :], grid_size)
    return turn_count.astype(jnp.float32) * (2.0 * math.pi / grid_size)

def forward_table(box_order, box_size, grid_size):
    angle_tab = phases(box_order, box_size, grid_size)
    cosine = jnp.cos(angle_tab) / math.sqrt(box_size)
    sine_part = jnp.sin(angle_tab) / math.sqrt(box_size)
    dft_table = jnp.stack([jnp.stack([cosine, sine_part], 1), jnp.stack([-sine_part, cosine], 1)], 0)
    return dft_table.astype(jnp.bfloat16)

def inverse_table(box_order, box_size, grid_size):
    angle_tab = phases(box_order, box_size, grid_size).T
    factor = math.sqrt(box_size) / grid_size
    cosine = jnp.cos(angle_tab) * factor
    sine_part = jnp.sin(angle_tab) * factor
    dft_table = jnp.stack([jnp.stack([cosine, -sine_part], 1), jnp.stack([sine_part, cosine], 1)], 0)
    return dft_table.astype(jnp.bfloat16)

def section_zy(coeff_block, table_z, table_y):
    leading = coeff_block.shape[0]
    planes = coeff_block.shape[1]
    split_up = coeff_block.reshape(leading, planes, W, 2, W)
    along_z = product('blyck,ckdn->blydn', split_up, table_z).astype(jnp.bfloat16)
    along_y = product('blycz,cydm->blmdz', along_z, table_y).astype(jnp.bfloat16)
    return along_y.reshape(leading, planes, G * 2 * G)

def section_x(arrived, table_x):
    leading = arrived.shape[0]
    y_rows = arrived.shape[2] // (2 * G)
    split_up = arrived.reshape(leading, W, y_rows, 2, G)
    return product('bxycz,cxdn->bnydz', split_up, table_x)

def section_x_inverse(weighted, table_x):
    leading = weighted.shape[0]
    y_rows = weighted.shape[2]
    along_x = product('bnydz,dncx->bxycz', weighted, table_x).astype(jnp.bfloat16)
    return along_x.reshape(leading, W, y_rows * 2 * G)

def section_zy_inverse(returned, table_y, table_z):
    leading = returned.shape[0]
    planes = returned.shape[1]
    split_up = returned.reshape(leading, planes, G, 2, G)
    along_y = product('blmdz,dmcy->blycz', split_up, table_y).astype(jnp.bfloat16)
    along_z = product('blydn,dnck->blyck', along_y, table_z)
    return along_z.reshape(leading, planes, W * 2 * W)

def wrap_offset(values):
    return jnp.mod(values + G // 2, G) - G // 2

def gaussians(coords, grid_cells):
    offset = wrap_offset(grid_cells[None, :] - coords[:, None]).astype(jnp.float32)
    return (jnp.exp(-offset * offset / (2.0 * sigma_cells * sigma_cells)), offset)

def atom_tables(own_pos, y_cells):
    grid_cells = jnp.arange(G, dtype=jnp.int32)
    gauss_x, offset_x = gaussians(own_pos[0], grid_cells)
    gauss_y, offset_y = gaussians(own_pos[1], y_cells)
    gauss_z, offset_z = gaussians(own_pos[2], grid_cells)
    return (gauss_x, offset_x, gauss_y, offset_y, gauss_z, offset_z)

def local_potential(tables, strength):
    gauss_x, offset_x, gauss_y, offset_y, gauss_z, offset_z = tables
    atom_count = gauss_x.shape[0]
    joined = (gauss_y[:, :, None] * gauss_z[:, None, :]).reshape(atom_count, -1)
    potential = jnp.dot((strength[:, None] * gauss_x).T, joined, precision=highest)
    return (potential, joined)

def atom_forces(density, tables, joined, strength):
    gauss_x, offset_x, gauss_y, offset_y, gauss_z, offset_z = tables
    atom_count = gauss_x.shape[0]
    with_y = ((gauss_y * offset_y)[:, :, None] * gauss_z[:, None, :]).reshape(atom_count, -1)
    with_z = (gauss_y[:, :, None] * (gauss_z * offset_z)[:, None, :]).reshape(atom_count, -1)
    stacked = jnp.concatenate([joined, with_y, with_z], 0)
    moments = jnp.dot(density, stacked.T, precision=highest)
    prefactor = -strength / (sigma_cells * sigma_cells)
    force_x = prefactor * lax.optimization_barrier(jnp.sum(gauss_x * offset_x * moments[:, :atom_count].T, 1))
    force_y = prefactor * lax.optimization_barrier(jnp.sum(gauss_x * moments[:, atom_count:2 * atom_count].T, 1))
    force_z = prefactor * lax.optimization_barrier(jnp.sum(gauss_x * moments[:, 2 * atom_count:].T, 1))
    return jnp.stack([force_x, force_y, force_z], 0)

def kinetic_table(x_cells):
    entries = jnp.arange(W * 2 * W, dtype=jnp.int32)
    wave_y = entries // (2 * W) - W // 2
    wave_z = jnp.mod(entries, W) - W // 2
    wave_x = x_cells - W // 2
    squared = wave_x[:, None] * wave_x[:, None] + (wave_y * wave_y + wave_z * wave_z)[None, :]
    return kinetic_scale * 0.5 * squared.astype(jnp.float32)

def rotate_quarter(values):
    leading = values.shape[0]
    middle = values.shape[1]
    split_up = values.reshape(leading, middle, W, 2, W)
    turned = jnp.stack([-split_up[:, :, :, 1, :], split_up[:, :, :, 0, :]], 3)
    return turned.reshape(values.shape)

def chain_forces(force, own_pos, before, after):
    ahead_step = wrap_offset(after - own_pos).astype(jnp.float32)
    behind = wrap_offset(own_pos - before).astype(jnp.float32)
    tangent_raw = ahead_step + behind
    entries = 3 * own_pos.shape[1]
    tangent = tangent_raw * lax.rsqrt(jnp.mean(tangent_raw * tangent_raw) + epsilon) / math.sqrt(entries)
    length_ahead = jnp.sqrt(entries * (jnp.mean(ahead_step * ahead_step) + epsilon))
    length_behind = jnp.sqrt(entries * (jnp.mean(behind * behind) + epsilon))
    along_path = jnp.sum(force * tangent)
    band_push = force - along_path * tangent + spring_constant * (length_ahead - length_behind) * tangent
    return (band_push, along_path)

def one_image(coeffs, rotation_one, own_pos, before, after, strength):
    flat_all = coeffs.reshape(BANDS, -1)
    orbitals = jnp.dot(rotation_one.T, flat_all, preferred_element_type=jnp.float32).astype(jnp.bfloat16)
    orbitals = orbitals.reshape(BLOCK, W, W * 2 * W)
    natural = jnp.arange(W, dtype=jnp.int32)
    table_f = forward_table(natural, W, G)
    table_i = inverse_table(natural, W, G)
    tables = atom_tables(own_pos, jnp.arange(G, dtype=jnp.int32))
    potential, joined = local_potential(tables, strength)
    grid_potential = potential.reshape(G, G, G)
    group_size = math.gcd(BLOCK, 16)
    blocks = orbitals.reshape(BLOCK // group_size, group_size, W, W * 2 * W)

    def apply_block(density, band_block):
        spread = section_zy(band_block, table_f, table_f)
        in_space = section_x(spread, table_f)
        density = density + lax.optimization_barrier(jnp.sum(in_space * in_space, axis=(0, 3)))
        weighted = (in_space * grid_potential[:, :, None, :]).astype(jnp.bfloat16)
        returned = section_x_inverse(weighted, table_i)
        return (density, section_zy_inverse(returned, table_i, table_i))
    density, applied = lax.scan(apply_block, jnp.zeros((G, G, G), jnp.float32), blocks)
    applied = applied.reshape(BLOCK, W, W * 2 * W)
    kinetic = kinetic_table(natural)
    orbitals_wide = orbitals.astype(jnp.float32)
    hamiltonian = kinetic[None] * orbitals_wide + applied
    numerator = lax.optimization_barrier(jnp.sum(orbitals_wide * hamiltonian, axis=(1, 2)))
    denominator = lax.optimization_barrier(jnp.sum(orbitals_wide * orbitals_wide, axis=(1, 2)))
    ritz_values = numerator / NPW / (denominator / NPW + epsilon)
    residual = hamiltonian - ritz_values[:, None, None] * orbitals_wide
    search = (residual / (1.0 + kinetic)[None]).astype(jnp.bfloat16)
    search_pair = jnp.concatenate([search.reshape(BLOCK, -1), (-rotate_quarter(search)).reshape(BLOCK, -1)], 0)
    intersections = jnp.dot(flat_all, search_pair.T, preferred_element_type=jnp.float32) / NPW
    intersections = intersections.astype(jnp.bfloat16)
    projected = jnp.dot(intersections.T, flat_all, preferred_element_type=jnp.float32)
    projection = projected[:BLOCK].reshape(BLOCK, W, -1) + rotate_quarter(projected[BLOCK:].reshape(BLOCK, W, -1))
    correction = (search.astype(jnp.float32) - projection).astype(jnp.bfloat16)
    atom_force = atom_forces((density / BLOCK).reshape(G, G * G), tables, joined, strength)
    band_push, along_path = chain_forces(atom_force, own_pos, before, after)
    return (correction, ritz_values, band_push, along_path)

def reference(coefficients, rotation, positions, start_pos, end_pos, species, depth):
    kind_ids = jnp.arange(SPECIES, dtype=jnp.int32)
    strength = lax.optimization_barrier(jnp.sum(jnp.where(species[:, None] == kind_ids[None, :], depth[None, :], 0.0), 1))
    results = []
    for image_idx in range(IMAGES):
        before = start_pos if image_idx == 0 else positions[image_idx - 1]
        after = end_pos if image_idx == IMAGES - 1 else positions[image_idx + 1]
        results.append(one_image(coefficients[image_idx], rotation[image_idx], positions[image_idx], before, after, strength))
    return (jnp.stack([entry_one[0] for entry_one in results], 0), jnp.stack([entry_one[1] for entry_one in results], 0), jnp.stack([entry_one[2] for entry_one in results], 0), jnp.stack([entry_one[3] for entry_one in results], 0))
```

```python
import math

import jax
import jax.numpy as jnp
import numpy as np
from jax import lax
from jax.experimental import pallas as pl
from jax.experimental.pallas import tpu as pltpu
from jax.sharding import PartitionSpec as P

G = 64
W = 32
BANDS = 1024
BLOCK = 256
SPECIES = 4


kinetic_scale = 0.01
sigma_cells = 3.0
spring_constant = 2.0
epsilon = 1e-06
highest = lax.Precision.HIGHEST


def passed_along(block, axis, distance):
    devices = range(lax.axis_size(axis))
    route = [(i - distance, i) for i in devices if i - distance in devices]
    return lax.ppermute(block, axis, route)


def phases():
    wavenum = np.arange(W, dtype=np.int32) - W // 2
    grid_cells = np.arange(G, dtype=np.int32)
    turn_count = np.mod(wavenum[:, None] * grid_cells[None, :], G)
    return turn_count.astype(np.float32) * np.float32(2.0 * math.pi / G)


def forward_table():
    angle_tab = phases()
    cosine = np.cos(angle_tab) / np.float32(math.sqrt(W))
    sine_part = np.sin(angle_tab) / np.float32(math.sqrt(W))
    return np.stack([np.stack([cosine, sine_part], 1), np.stack([-sine_part, cosine], 1)], 0)


def inverse_table():
    angle_tab = phases().T
    factor = np.float32(math.sqrt(W) / G)
    cosine = np.cos(angle_tab) * factor
    sine_part = np.sin(angle_tab) * factor
    return np.stack([np.stack([cosine, -sine_part], 1), np.stack([sine_part, cosine], 1)], 0)


def kernel_tables():
    fwd = forward_table()
    inv = inverse_table()
    two = np.eye(2, dtype=np.float32)
    table_z = np.einsum("czdn,vw,ij->jviczdwn", fwd, two, two).reshape(2, 8 * W, 4 * G)
    back_z = np.einsum("dncz,vw,ij->jdwnvicz", inv, two, two).reshape(2, 4 * G, 8 * W)
    fwd_y = fwd.reshape(2, W // 2, 2, 2, G)
    table_y = np.einsum("dgpem->empdg", fwd_y).reshape(2 * G, 2 * W)
    table_x = np.einsum("dxem->emxd", fwd).reshape(2 * G, 2 * W)
    back_x = np.einsum("emdx->xdem", inv).reshape(2 * W, 2 * G)
    inv_y = inv.reshape(2, G, 2, W // 2, 2)
    back_y = np.einsum("dmcgp->pcgdm", inv_y).reshape(2 * W, 2 * G)
    listed = (table_z, table_y, table_x, back_x, back_y, back_z)
    return [jnp.asarray(t, dtype=jnp.bfloat16) for t in listed]


def kinetic_table():
    wave = np.arange(W, dtype=np.int32) - W // 2
    sq = wave * wave
    squared = sq[:, None, None, None] + sq[None, :, None, None] + sq[None, None, None, :]
    squared = np.broadcast_to(squared, (W, W, 2, W)).reshape(W * W // 2, 4 * W)
    return np.float32(kinetic_scale * 0.5) * squared.astype(np.float32)


def mm(left, right):
    return jnp.dot(left, right, preferred_element_type=jnp.float32)


MESH_ID = pl.DeviceIdType.MESH
GROUP = ("band", "pw")


def group_place():
    inner = lax.axis_size(GROUP[1])
    count = lax.axis_size(GROUP[0]) * inner
    mine = lax.axis_index(GROUP[0]) * inner + lax.axis_index(GROUP[1])
    return mine, count, inner


def device_of(index, inner):
    return {GROUP[0]: index // inner, GROUP[1]: lax.rem(index, inner)}


def greet_all(mine, count, inner):
    barrier = pltpu.get_barrier_semaphore()
    for k in range(1, count):
        peer = lax.rem(mine + k, count)
        pl.semaphore_signal(
            barrier, inc=1, device_id=device_of(peer, inner), device_id_type=MESH_ID
        )
    pl.semaphore_wait(barrier, count - 1)


def apply_kernel(
    orb_ref, pot_ref, kin_ref, tz_ref, ty_ref, tx_ref, bx_ref, by_ref, bz_ref,
    out_ref, ritz_ref, dens_ref,
    in_ref, back_ref, zs_ref, s_ref, send_sem, recv_sem, back_send_sem, back_recv_sem,
):
    lanes = 2 * G
    half = W // 2
    rows = W * half
    bf = jnp.bfloat16
    mine, count, inner = group_place()
    chunks = orb_ref.shape[1] // 2

    greet_all(mine, count, inner)

    def send_chunk(c, carry):
        at = pl.ds(2 * c, 2)
        for k in range(1, count):
            peer = lax.rem(mine + k, count)
            pltpu.make_async_remote_copy(
                src_ref=orb_ref.at[peer, at],
                dst_ref=in_ref.at[mine, at],
                send_sem=send_sem.at[c],
                recv_sem=recv_sem.at[c],
                device_id=device_of(peer, inner),
                device_id_type=MESH_ID,
            ).start()
        return carry

    lax.fori_loop(0, chunks, send_chunk, 0)
    in_ref[mine] = orb_ref[mine]
    dens_ref[...] = jnp.zeros_like(dens_ref)

    def all_of(ref, c, sem):
        part = ref.at[pl.ds(0, count - 1), pl.ds(2 * c, 2)]
        return pltpu.make_async_copy(part, part, sem.at[c])

    def chunk_step(c, chunk_carry):
        all_of(in_ref, c, recv_sem).wait()
        vecs = jnp.concatenate(
            [in_ref[:, 2 * c + v].reshape(rows, 4 * W) for v in range(2)], axis=1
        )
        for p in range(2):
            zs_ref[p] = mm(vecs, tz_ref[p]).astype(bf)

        def y_step(i, carry):
            cols = []
            for k in range(2):
                at = pl.ds(pl.multiple_of((2 * i + k) * half, half), half)
                parts = [
                    zs_ref[p, at, d * lanes : (d + 1) * lanes] for p in range(2) for d in range(2)
                ]
                cols.append(jnp.concatenate(parts, axis=0))
            done = mm(ty_ref[...], jnp.concatenate(cols, axis=1))
            for k in range(2):
                at = pl.ds(pl.multiple_of((2 * i + k) * lanes, lanes), lanes)
                s_ref[at, :] = done[:, k * lanes : (k + 1) * lanes]
            return carry

        lax.fori_loop(0, W // 2, y_step, 0, unroll=4)

        def x_step(i, carry):
            ats = [pl.ds(2 * i + k, 2 * W, stride=G) for k in range(2)]
            cols = [s_ref[at, :].astype(bf) for at in ats]
            done = mm(tx_ref[...], jnp.concatenate(cols, axis=1))
            real, imag = (done[:G], done[G:])
            pot = jnp.concatenate([pot_ref[2 * i], pot_ref[2 * i + 1]], axis=1)
            square = real * real + imag * imag
            for k in range(2):
                dens_ref[2 * i + k] += square[:, k * lanes : (k + 1) * lanes]
            weighted = jnp.concatenate([(real * pot).astype(bf), (imag * pot).astype(bf)], axis=0)
            back = mm(bx_ref[...], weighted)
            for k in range(2):
                s_ref[ats[k], :] = back[:, k * lanes : (k + 1) * lanes]
            return carry

        lax.fori_loop(0, G // 2, x_step, 0, unroll=4)

        def back_y_step(i, carry):
            cols = []
            for k in range(2):
                at = pl.ds(pl.multiple_of((2 * i + k) * lanes, lanes), lanes)
                cols.append(s_ref[at, :].astype(bf))
            done = mm(by_ref[...], jnp.concatenate(cols, axis=1)).astype(bf)
            for k in range(2):
                at = pl.ds(pl.multiple_of((2 * i + k) * half, half), half)
                for p in range(2):
                    for q in range(2):
                        r = (2 * p + q) * half
                        zs_ref[p, at, q * lanes : (q + 1) * lanes] = done[
                            r : r + half, k * lanes : (k + 1) * lanes
                        ]
            return carry

        lax.fori_loop(0, W // 2, back_y_step, 0, unroll=4)

        local = mm(zs_ref[0], bz_ref[0]) + mm(zs_ref[1], bz_ref[1])
        kin = kin_ref[...]
        npw_total = W * W * W
        for v in range(2):
            orb = in_ref[:, 2 * c + v].reshape(rows, 4 * W).astype(jnp.float32)
            ham = kin * orb + local[:, v * 4 * W : (v + 1) * 4 * W]
            numerator = jnp.sum(jnp.sum(orb * ham, axis=0, keepdims=True), axis=1, keepdims=True)
            denominator = jnp.sum(jnp.sum(orb * orb, axis=0, keepdims=True), axis=1, keepdims=True)
            ritz = numerator / npw_total / (denominator / npw_total + epsilon)
            search = ((ham - ritz * orb) / (1.0 + kin)).astype(bf)
            back_ref[:, 2 * c + v] = search.reshape(in_ref.shape[0], *in_ref.shape[2:])
            ritz_ref[c, :, v * 128 : (v + 1) * 128] = jnp.broadcast_to(ritz, (8, 128))
        at = pl.ds(2 * c, 2)
        out_ref[mine, at] = back_ref[mine, at]
        for k in range(1, count):
            peer = lax.rem(mine + k, count)
            pltpu.make_async_remote_copy(
                src_ref=back_ref.at[peer, at],
                dst_ref=out_ref.at[mine, at],
                send_sem=back_send_sem.at[c],
                recv_sem=back_recv_sem.at[c],
                device_id=device_of(peer, inner),
                device_id_type=MESH_ID,
            ).start()
        return chunk_carry

    lax.fori_loop(0, chunks, chunk_step, 0)

    def finish(c, carry):
        all_of(in_ref, c, send_sem).wait()
        all_of(out_ref, c, back_send_sem).wait()
        all_of(out_ref, c, back_recv_sem).wait()
        return carry

    lax.fori_loop(0, chunks, finish, 0)


def apply_all(orbitals, potential):
    devices, vectors, planes, half, lanes = orbitals.shape
    tabs = kernel_tables()
    kin = jnp.asarray(kinetic_table())
    whole = pl.BlockSpec(memory_space=pltpu.VMEM)
    chunks = vectors // 2
    flops = vectors * 2 * 2 * (W * W * 2 * W * 2 * G + W * G * 2 * W * 2 * G + G * G * 2 * W * 2 * G)
    return pl.pallas_call(
        apply_kernel,
        in_specs=[whole] * 9,
        out_specs=[whole] * 3,
        out_shape=[
            jax.ShapeDtypeStruct(orbitals.shape, jnp.bfloat16),
            jax.ShapeDtypeStruct((chunks, 8, 256), jnp.float32),
            jax.ShapeDtypeStruct((G, G, 2 * G), jnp.float32),
        ],
        scratch_shapes=[
            pltpu.VMEM(orbitals.shape, jnp.bfloat16),
            pltpu.VMEM(orbitals.shape, jnp.bfloat16),
            pltpu.VMEM((2, W * W // 2, 4 * G), jnp.bfloat16),
            pltpu.VMEM((W * 2 * G, 2 * G), jnp.float32),
            pltpu.SemaphoreType.DMA((chunks,)),
            pltpu.SemaphoreType.DMA((chunks,)),
            pltpu.SemaphoreType.DMA((chunks,)),
            pltpu.SemaphoreType.DMA((chunks,)),
        ],
        compiler_params=pltpu.CompilerParams(
            collective_id=0, has_side_effects=True, vmem_limit_bytes=44 * 1024 * 1024
        ),
        cost_estimate=pl.CostEstimate(flops=flops, bytes_accessed=8 << 20, transcendentals=0),
        name="apply_all",
    )(orbitals, potential, kin, *tabs)


def turn_kernel(c_ref, r_ref, out_ref):
    block = c_ref[...]
    out_ref[0] = block
    size = r_ref.shape[0]
    for t in range(block.shape[1] // size):
        at = slice(t * size, (t + 1) * size)
        out_ref[1, :, at] = mm(block[:, at], r_ref[...]).astype(jnp.bfloat16)


def with_turned(flat_all):
    bands, entries = flat_all.shape
    one = np.zeros((2, W, 2, W), np.float32)
    one[1, :, 0, :] = -np.eye(W)
    one[0, :, 1, :] = np.eye(W)
    turn = np.kron(np.eye(4, dtype=np.float32), one.reshape(2 * W, 2 * W))
    turn = jnp.asarray(turn, dtype=jnp.bfloat16)
    tile = 256
    return pl.pallas_call(
        turn_kernel,
        grid=(bands // tile,),
        in_specs=[
            pl.BlockSpec((tile, entries), lambda p: (p, 0)),
            pl.BlockSpec(turn.shape, lambda p: (0, 0)),
        ],
        out_specs=pl.BlockSpec((2, tile, entries), lambda p: (0, p, 0)),
        out_shape=jax.ShapeDtypeStruct((2, bands, entries), jnp.bfloat16),
        compiler_params=pltpu.CompilerParams(
            dimension_semantics=("arbitrary",), vmem_limit_bytes=40 * 1024 * 1024
        ),
        cost_estimate=pl.CostEstimate(
            flops=2 * bands * entries * 256, bytes_accessed=6 * bands * entries, transcendentals=0
        ),
        name="with_turned",
    )(flat_all, turn)


def wrap_offset(values):
    return jnp.mod(values + G // 2, G) - G // 2


def gaussians(coords, grid_cells):
    offset = wrap_offset(grid_cells[None, :] - coords[:, None]).astype(jnp.float32)
    return (jnp.exp(-offset * offset / (2.0 * sigma_cells * sigma_cells)), offset)


def atom_tables(own_pos, y_cells):
    grid_cells = jnp.arange(G, dtype=jnp.int32)
    gauss_x, offset_x = gaussians(own_pos[0], grid_cells)
    gauss_y, offset_y = gaussians(own_pos[1], y_cells)
    gauss_z, offset_z = gaussians(own_pos[2], grid_cells)
    return (gauss_x, offset_x, gauss_y, offset_y, gauss_z, offset_z)


def local_potential(tables, strength):
    gauss_x, offset_x, gauss_y, offset_y, gauss_z, offset_z = tables
    atom_count = gauss_x.shape[0]
    joined = (gauss_y[:, :, None] * gauss_z[:, None, :]).reshape(atom_count, -1)
    potential = jnp.dot((strength[:, None] * gauss_x).T, joined, precision=highest)
    return (potential, joined)


def atom_forces(density, tables, joined, strength):
    gauss_x, offset_x, gauss_y, offset_y, gauss_z, offset_z = tables
    atom_count = gauss_x.shape[0]
    with_y = ((gauss_y * offset_y)[:, :, None] * gauss_z[:, None, :]).reshape(atom_count, -1)
    with_z = (gauss_y[:, :, None] * (gauss_z * offset_z)[:, None, :]).reshape(atom_count, -1)
    stacked = jnp.concatenate([joined, with_y, with_z], 0)
    moments = jnp.dot(density, stacked.T, precision=highest)
    prefactor = -strength / (sigma_cells * sigma_cells)
    force_x = prefactor * jnp.sum(gauss_x * offset_x * moments[:, :atom_count].T, 1)
    force_y = prefactor * jnp.sum(gauss_x * moments[:, atom_count : 2 * atom_count].T, 1)
    force_z = prefactor * jnp.sum(gauss_x * moments[:, 2 * atom_count :].T, 1)
    return jnp.stack([force_x, force_y, force_z], 0)


def chain_forces(force, own_pos, before, after):
    ahead_step = wrap_offset(after - own_pos).astype(jnp.float32)
    behind = wrap_offset(own_pos - before).astype(jnp.float32)
    tangent_raw = ahead_step + behind
    entries = 3 * own_pos.shape[1]
    tangent = (
        tangent_raw * lax.rsqrt(jnp.mean(tangent_raw * tangent_raw) + epsilon) / math.sqrt(entries)
    )
    length_ahead = jnp.sqrt(entries * (jnp.mean(ahead_step * ahead_step) + epsilon))
    length_behind = jnp.sqrt(entries * (jnp.mean(behind * behind) + epsilon))
    along_path = jnp.sum(force * tangent)
    band_push = (
        force - along_path * tangent + spring_constant * (length_ahead - length_behind) * tangent
    )
    return (band_push, along_path)


def body(coefficients, rotation, positions, start_pos, end_pos, species, depth):
    axes = ("band", "pw")
    devices = lax.axis_size(axes)
    coeff_all = coefficients[0]
    planes = coeff_all.shape[1]
    flat_all = coeff_all.reshape(BANDS, -1)
    vectors = BLOCK // devices
    orbitals = jnp.einsum("ib,ik->bk", rotation[0], flat_all, preferred_element_type=jnp.float32)
    orbitals = orbitals.astype(jnp.bfloat16).reshape(BLOCK, planes * (W // 2), 4 * W)
    orbitals = orbitals.reshape(devices, vectors, planes, W // 2, 4 * W)
    both = with_turned(flat_all)
    kind_ids = jnp.arange(SPECIES, dtype=jnp.int32)
    strength = jnp.sum(jnp.where(species[:, None] == kind_ids[None, :], depth[None, :], 0.0), 1)
    own_pos = positions[0]
    tables = atom_tables(own_pos, jnp.arange(G, dtype=jnp.int32))
    potential, joined = local_potential(tables, strength)
    potential = jnp.swapaxes(potential.reshape(G, G, G), 0, 1)
    potential = jnp.concatenate([potential, potential], 2)
    search, ritz, density = apply_all(orbitals, potential)
    search = search.reshape(BLOCK, -1)
    density = jnp.swapaxes(density[:, :, :G] + density[:, :, G:], 0, 1).reshape(G, G * G) / BLOCK
    force_part = atom_forces(density, tables, joined, strength)
    own_ritz = ritz[:, 0, ::128].reshape(vectors)
    ritz_part = lax.dynamic_update_slice(
        jnp.zeros((BLOCK,), jnp.float32), own_ritz, (lax.axis_index(axes) * vectors,)
    )
    summed = lax.psum(jnp.concatenate([force_part.reshape(-1), ritz_part]), axes)
    atom_force = summed[: force_part.size].reshape(force_part.shape)
    ritz_values = summed[force_part.size :]
    npw_total = W * W * W
    stacked = both.reshape(2 * BANDS, -1)
    partial = jnp.einsum("ik,jk->ij", stacked, search, preferred_element_type=jnp.float32)
    partial = (partial / npw_total).astype(jnp.bfloat16)
    arrived = lax.all_to_all(partial, axes, split_axis=0, concat_axis=0, tiled=True)
    arrived = arrived.reshape(devices, 2 * BANDS // devices, BLOCK).astype(jnp.float32)
    own_sum = jnp.sum(arrived, 0).astype(jnp.bfloat16)
    intersections = lax.all_gather(own_sum, axes, axis=0, tiled=True)
    projection = jnp.einsum(
        "ij,ik->jk", intersections, stacked, preferred_element_type=jnp.float32
    )
    correction = (search.astype(jnp.float32) - projection).astype(jnp.bfloat16)
    correction = correction.reshape(BLOCK, planes, W * 2 * W)
    image_idx = lax.axis_index("img")
    before = passed_along(own_pos, "img", 1)
    after = passed_along(own_pos, "img", -1)
    before = jnp.where(image_idx == 0, start_pos, before)
    after = jnp.where(image_idx == lax.axis_size("img") - 1, end_pos, after)
    band_push, along_path = chain_forces(atom_force, own_pos, before, after)
    return (correction[None], ritz_values[None], band_push[None], along_path[None])


def solution(mesh):
    in_specs = (
        P("img", None, ("band", "pw"), None),
        P("img", None, None),
        P("img", None, None),
        P(),
        P(),
        P(),
        P(),
    )
    out_specs = (
        P("img", None, ("band", "pw"), None),
        P("img", None),
        P("img", None, None),
        P("img"),
    )
    return jax.shard_map(body, mesh=mesh, in_specs=in_specs, out_specs=out_specs, check_vma=False)
```

```python
import math

import jax
import jax.numpy as jnp
import numpy as np
from jax import lax
from jax.experimental import pallas as pl
from jax.experimental.pallas import tpu as pltpu
from jax.sharding import PartitionSpec as P

G = 64
W = 32
BANDS = 1024
BLOCK = 256
SPECIES = 4


kinetic_scale = 0.01
sigma_cells = 3.0
spring_constant = 2.0
epsilon = 1e-06
highest = lax.Precision.HIGHEST


def passed_along(block, axis, distance):
    devices = range(lax.axis_size(axis))
    route = [(i - distance, i) for i in devices if i - distance in devices]
    return lax.ppermute(block, axis, route)


def phases():
    wavenum = np.arange(W, dtype=np.int32) - W // 2
    grid_cells = np.arange(G, dtype=np.int32)
    turn_count = np.mod(wavenum[:, None] * grid_cells[None, :], G)
    return turn_count.astype(np.float32) * np.float32(2.0 * math.pi / G)


def forward_table():
    angle_tab = phases()
    cosine = np.cos(angle_tab) / np.float32(math.sqrt(W))
    sine_part = np.sin(angle_tab) / np.float32(math.sqrt(W))
    return np.stack([np.stack([cosine, sine_part], 1), np.stack([-sine_part, cosine], 1)], 0)


def inverse_table():
    angle_tab = phases().T
    factor = np.float32(math.sqrt(W) / G)
    cosine = np.cos(angle_tab) * factor
    sine_part = np.sin(angle_tab) * factor
    return np.stack([np.stack([cosine, -sine_part], 1), np.stack([sine_part, cosine], 1)], 0)


def kernel_tables():
    fwd = forward_table()
    inv = inverse_table()
    two = np.eye(2, dtype=np.float32)
    table_z = np.einsum("czdn,vw,ij->jviczdwn", fwd, two, two).reshape(2, 8 * W, 4 * G)
    back_z = np.einsum("dncz,vw,ij->jdwnvicz", inv, two, two).reshape(2, 4 * G, 8 * W)
    fwd_y = fwd.reshape(2, W // 2, 2, 2, G)
    table_y = np.einsum("dgpem->empdg", fwd_y).reshape(2 * G, 2 * W)
    table_x = np.einsum("dxem->emxd", fwd).reshape(2 * G, 2 * W)
    back_x = np.einsum("emdx->xdem", inv).reshape(2 * W, 2 * G)
    inv_y = inv.reshape(2, G, 2, W // 2, 2)
    back_y = np.einsum("dmcgp->pcgdm", inv_y).reshape(2 * W, 2 * G)
    listed = (table_z, table_y, table_x, back_x, back_y, back_z)
    return [jnp.asarray(t, dtype=jnp.bfloat16) for t in listed]


def kinetic_table():
    wave = np.arange(W, dtype=np.int32) - W // 2
    sq = wave * wave
    squared = sq[:, None, None, None] + sq[None, :, None, None] + sq[None, None, None, :]
    squared = np.broadcast_to(squared, (W, W, 2, W)).reshape(W * W // 2, 4 * W)
    return np.float32(kinetic_scale * 0.5) * squared.astype(np.float32)


def mm(left, right):
    return jnp.dot(left, right, preferred_element_type=jnp.float32)


MESH_ID = pl.DeviceIdType.MESH
GROUP = ("band", "pw")


def group_place():
    inner = lax.axis_size(GROUP[1])
    count = lax.axis_size(GROUP[0]) * inner
    mine = lax.axis_index(GROUP[0]) * inner + lax.axis_index(GROUP[1])
    return mine, count, inner


def device_of(index, inner):
    return {GROUP[0]: index // inner, GROUP[1]: lax.rem(index, inner)}


def greet_all(mine, count, inner):
    barrier = pltpu.get_barrier_semaphore()
    for k in range(1, count):
        peer = lax.rem(mine + k, count)
        pl.semaphore_signal(
            barrier, inc=1, device_id=device_of(peer, inner), device_id_type=MESH_ID
        )
    pl.semaphore_wait(barrier, count - 1)


def apply_kernel(
    orb_ref, pot_ref, kin_ref, tz_ref, ty_ref, tx_ref, bx_ref, by_ref, bz_ref,
    out_ref, ritz_ref, dens_ref,
    in_ref, back_ref, zs_ref, s_ref, send_sem, recv_sem, back_send_sem, back_recv_sem,
):
    lanes = 2 * G
    half = W // 2
    rows = W * half
    bf = jnp.bfloat16
    mine, count, inner = group_place()
    chunks = orb_ref.shape[1] // 2

    greet_all(mine, count, inner)

    def send_chunk(c, carry):
        at = pl.ds(2 * c, 2)
        for k in range(1, count):
            peer = lax.rem(mine + k, count)
            pltpu.make_async_remote_copy(
                src_ref=orb_ref.at[peer, at],
                dst_ref=in_ref.at[mine, at],
                send_sem=send_sem.at[c],
                recv_sem=recv_sem.at[c],
                device_id=device_of(peer, inner),
                device_id_type=MESH_ID,
            ).start()
        return carry

    lax.fori_loop(0, chunks, send_chunk, 0)
    in_ref[mine] = orb_ref[mine]
    dens_ref[...] = jnp.zeros_like(dens_ref)
    ritz_ref[...] = jnp.zeros_like(ritz_ref)

    def all_of(ref, c, sem):
        part = ref.at[pl.ds(0, count - 1), pl.ds(2 * c, 2)]
        return pltpu.make_async_copy(part, part, sem.at[c])

    def chunk_step(c, chunk_carry):
        all_of(in_ref, c, recv_sem).wait()
        vecs = jnp.concatenate(
            [in_ref[:, 2 * c + v].reshape(rows, 4 * W) for v in range(2)], axis=1
        )
        for p in range(2):
            zs_ref[p] = mm(vecs, tz_ref[p]).astype(bf)

        def y_step(i, carry):
            cols = []
            for k in range(2):
                at = pl.ds(pl.multiple_of((2 * i + k) * half, half), half)
                parts = [
                    zs_ref[p, at, d * lanes : (d + 1) * lanes] for p in range(2) for d in range(2)
                ]
                cols.append(jnp.concatenate(parts, axis=0))
            done = mm(ty_ref[...], jnp.concatenate(cols, axis=1))
            for k in range(2):
                at = pl.ds(pl.multiple_of((2 * i + k) * lanes, lanes), lanes)
                s_ref[at, :] = done[:, k * lanes : (k + 1) * lanes]
            return carry

        lax.fori_loop(0, W // 2, y_step, 0, unroll=4)

        def x_step(i, carry):
            ats = [pl.ds(2 * i + k, 2 * W, stride=G) for k in range(2)]
            cols = [s_ref[at, :].astype(bf) for at in ats]
            done = mm(tx_ref[...], jnp.concatenate(cols, axis=1))
            real, imag = (done[:G], done[G:])
            pot = jnp.concatenate([pot_ref[2 * i], pot_ref[2 * i + 1]], axis=1)
            square = real * real + imag * imag
            for k in range(2):
                dens_ref[2 * i + k] += square[:, k * lanes : (k + 1) * lanes]
            weighted = jnp.concatenate([(real * pot).astype(bf), (imag * pot).astype(bf)], axis=0)
            back = mm(bx_ref[...], weighted)
            for k in range(2):
                s_ref[ats[k], :] = back[:, k * lanes : (k + 1) * lanes]
            return carry

        lax.fori_loop(0, G // 2, x_step, 0, unroll=4)

        def back_y_step(i, carry):
            cols = []
            for k in range(2):
                at = pl.ds(pl.multiple_of((2 * i + k) * lanes, lanes), lanes)
                cols.append(s_ref[at, :].astype(bf))
            done = mm(by_ref[...], jnp.concatenate(cols, axis=1)).astype(bf)
            for k in range(2):
                at = pl.ds(pl.multiple_of((2 * i + k) * half, half), half)
                for p in range(2):
                    for q in range(2):
                        r = (2 * p + q) * half
                        zs_ref[p, at, q * lanes : (q + 1) * lanes] = done[
                            r : r + half, k * lanes : (k + 1) * lanes
                        ]
            return carry

        lax.fori_loop(0, W // 2, back_y_step, 0, unroll=4)

        local = mm(zs_ref[0], bz_ref[0]) + mm(zs_ref[1], bz_ref[1])
        kin = kin_ref[...]
        npw_total = W * W * W
        for v in range(2):
            orb = in_ref[:, 2 * c + v].reshape(rows, 4 * W).astype(jnp.float32)
            ham = kin * orb + local[:, v * 4 * W : (v + 1) * 4 * W]
            numerator = jnp.sum(jnp.sum(orb * ham, axis=0, keepdims=True), axis=1, keepdims=True)
            denominator = jnp.sum(jnp.sum(orb * orb, axis=0, keepdims=True), axis=1, keepdims=True)
            ritz = numerator / npw_total / (denominator / npw_total + epsilon)
            search = ((ham - ritz * orb) / (1.0 + kin)).astype(bf)
            back_ref[:, 2 * c + v] = search.reshape(in_ref.shape[0], *in_ref.shape[2:])
            slot = lax.broadcasted_iota(jnp.int32, ritz_ref.shape, 1)
            here = slot == mine * orb_ref.shape[1] + 2 * c + v
            ritz_ref[...] = jnp.where(here, ritz, ritz_ref[...])
        at = pl.ds(2 * c, 2)
        out_ref[mine, at] = back_ref[mine, at]
        for k in range(1, count):
            peer = lax.rem(mine + k, count)
            pltpu.make_async_remote_copy(
                src_ref=back_ref.at[peer, at],
                dst_ref=out_ref.at[mine, at],
                send_sem=back_send_sem.at[c],
                recv_sem=back_recv_sem.at[c],
                device_id=device_of(peer, inner),
                device_id_type=MESH_ID,
            ).start()
        return chunk_carry

    lax.fori_loop(0, chunks, chunk_step, 0)

    def finish(c, carry):
        all_of(in_ref, c, send_sem).wait()
        all_of(out_ref, c, back_send_sem).wait()
        all_of(out_ref, c, back_recv_sem).wait()
        return carry

    lax.fori_loop(0, chunks, finish, 0)


def apply_all(orbitals, potential):
    devices, vectors, planes, half, lanes = orbitals.shape
    tabs = kernel_tables()
    kin = jnp.asarray(kinetic_table())
    whole = pl.BlockSpec(memory_space=pltpu.VMEM)
    chunks = vectors // 2
    flops = vectors * 2 * 2 * (W * W * 2 * W * 2 * G + W * G * 2 * W * 2 * G + G * G * 2 * W * 2 * G)
    return pl.pallas_call(
        apply_kernel,
        in_specs=[whole] * 9,
        out_specs=[whole] * 3,
        out_shape=[
            jax.ShapeDtypeStruct(orbitals.shape, jnp.bfloat16),
            jax.ShapeDtypeStruct((8, BLOCK), jnp.float32),
            jax.ShapeDtypeStruct((G, G, 2 * G), jnp.float32),
        ],
        scratch_shapes=[
            pltpu.VMEM(orbitals.shape, jnp.bfloat16),
            pltpu.VMEM(orbitals.shape, jnp.bfloat16),
            pltpu.VMEM((2, W * W // 2, 4 * G), jnp.bfloat16),
            pltpu.VMEM((W * 2 * G, 2 * G), jnp.float32),
            pltpu.SemaphoreType.DMA((chunks,)),
            pltpu.SemaphoreType.DMA((chunks,)),
            pltpu.SemaphoreType.DMA((chunks,)),
            pltpu.SemaphoreType.DMA((chunks,)),
        ],
        compiler_params=pltpu.CompilerParams(
            collective_id=0, has_side_effects=True, vmem_limit_bytes=44 * 1024 * 1024
        ),
        cost_estimate=pl.CostEstimate(flops=flops, bytes_accessed=8 << 20, transcendentals=0),
        name="apply_all",
    )(orbitals, potential, kin, *tabs)


def atom_rows(pos_ref, axis):
    cell = lax.broadcasted_iota(jnp.int32, (G, pos_ref.shape[1]), 0)
    shifted = (cell - pos_ref[axis : axis + 1, :] + G // 2) & (G - 1)
    offset = (shifted - G // 2).astype(jnp.float32)
    return jnp.exp(-offset * offset / (2.0 * sigma_cells * sigma_cells)), offset


def split_two(values):
    high = values.astype(jnp.bfloat16)
    return high, (values - high.astype(jnp.float32)).astype(jnp.bfloat16)


def quarter_turn(values, sign):
    lane = lax.broadcasted_iota(jnp.int32, values.shape, 1)
    first = (lane // W) % 2 == 0
    size = values.shape[1]
    later = pltpu.roll(values, size - W, 1)
    earlier = pltpu.roll(values, W, 1)
    return jnp.where(first, sign * later, -sign * earlier)


def partial_forces(dens_ref, pos_ref, strength_ref, gy_ref, gyd_ref, f_ref):
    atoms = pos_ref.shape[1]
    gauss_x, offset_x = atom_rows(pos_ref, 0)
    gauss_y, offset_y = atom_rows(pos_ref, 1)
    gauss_z, offset_z = atom_rows(pos_ref, 2)
    gy_ref[...] = gauss_y
    gyd_ref[...] = gauss_y * offset_y
    high, low = split_two(jnp.concatenate([gauss_z, gauss_z * offset_z], axis=1))
    table = jnp.concatenate([high, high, low, jnp.zeros_like(low)], axis=0)
    f_ref[...] = jnp.zeros_like(f_ref)
    group = 4
    left = lax.broadcasted_iota(jnp.int32, (G, 2 * G), 1) < G

    def step(i, carry):
        rows = []
        for k in range(group):
            pair = dens_ref[group * i + k]
            both = (pair + pltpu.roll(pair, G, 1)) * (1.0 / BLOCK)
            high_part = both.astype(jnp.bfloat16).astype(jnp.float32)
            rest = both - high_part
            rows.append(
                jnp.concatenate(
                    [jnp.where(left, high_part, rest), jnp.where(left, high_part, 0.0)], axis=1
                ).astype(jnp.bfloat16)
            )
        done = mm(jnp.concatenate(rows, axis=0), table)
        sums = [f_ref[m] for m in range(3)]
        for k in range(group):
            plain = done[k * G : (k + 1) * G, :atoms]
            along = done[k * G : (k + 1) * G, atoms:]
            at = pl.ds(group * i + k, 1)
            gauss = gy_ref[at, :]
            sums[0] += gauss * plain
            sums[1] += gyd_ref[at, :] * plain
            sums[2] += gauss * along
        for m in range(3):
            f_ref[m] = sums[m]
        return carry

    lax.fori_loop(0, G // group, step, 0)
    prefactor = -strength_ref[...] / (sigma_cells * sigma_cells)
    weights = [gauss_x * offset_x, gauss_x, gauss_x]
    return [prefactor * jnp.sum(weights[m] * f_ref[m], axis=0, keepdims=True) for m in range(3)]


def project_kernel(
    c_ref, search_ref, dens_ref, ritz_in_ref, pos_ref, strength_ref,
    out_ref, small_ref,
    wide_ref, pair_ref, part_ref, got_ref, mid_ref, got2_ref, all_ref, proj_ref, acc_ref,
    own_small_ref, smalls_ref, gy_ref, gyd_ref, f_ref,
    send1, recv1, send2, recv2, send_z, recv_z, send_xy, recv_xy, send_s, recv_s,
):
    bf = jnp.bfloat16
    mine, count, inner = group_place()
    outer = count // inner
    me_outer, me_inner = lax.axis_index(GROUP[0]), lax.axis_index(GROUP[1])
    bands, entries = c_ref.shape
    npw_total = W * W * W
    lanes = 4 * W
    blocks = entries // lanes
    per_inner = bands // inner
    two = 2 * BLOCK
    per_outer = two // outer

    greet_all(mine, count, inner)

    def widen(i, carry):
        size = search_ref.shape[1] * blocks
        at = pl.ds(pl.multiple_of(i * size, size), size)
        wide_ref[at, :] = search_ref[i].reshape(size, lanes).astype(jnp.float32)
        return carry

    lax.fori_loop(0, count, widen, 0)

    def lay(j, carry):
        block = wide_ref[pl.ds(j, BLOCK, stride=blocks), :]
        at = pl.ds(pl.multiple_of(j * lanes, lanes), lanes)
        pair_ref[:BLOCK, at] = block.astype(bf)
        pair_ref[BLOCK:, at] = quarter_turn(block, 1.0).astype(bf)
        return carry

    lax.fori_loop(0, blocks, lay, 0)

    depth = 1024

    def overlap(quarter):
        rows = pl.ds(pl.multiple_of(quarter * per_inner, per_inner), per_inner)
        acc_ref[...] = jnp.zeros_like(acc_ref)

        def step(i, carry):
            at = pl.ds(pl.multiple_of(i * depth, depth), depth)
            acc_ref[...] += lax.dot_general(
                pair_ref[:, at], c_ref[rows, at], (((1,), (1,)), ((), ())),
                preferred_element_type=jnp.float32,
            )
            return carry

        lax.fori_loop(0, entries // depth, step, 0)

    def to_inner(k):
        return lax.rem(me_inner + k, inner)

    def to_outer(k):
        return lax.rem(me_outer + k, outer)

    def remote(src, dst, send, recv, where):
        return pltpu.make_async_remote_copy(
            src_ref=src, dst_ref=dst, send_sem=send, recv_sem=recv,
            device_id=where, device_id_type=MESH_ID,
        )

    def first_copy(k):
        quarter = to_inner(k)
        return remote(
            part_ref.at[quarter], got_ref.at[me_inner], send1.at[k], recv1.at[k], {GROUP[1]: quarter}
        )

    def send_quarter(k, carry):
        quarter = to_inner(k)
        overlap(quarter)
        part_ref[quarter] = (acc_ref[...] / npw_total).astype(bf)
        first_copy(k).start()
        return carry

    lax.fori_loop(1, inner, send_quarter, 0)
    overlap(me_inner)

    forces = partial_forces(dens_ref, pos_ref, strength_ref, gy_ref, gyd_ref, f_ref)
    own_small_ref[...] = ritz_in_ref[...]
    for m in range(3):
        own_small_ref[m + 1 : m + 2, :] = forces[m]

    def small_copy(k):
        peer = lax.rem(mine + k, count)
        return remote(
            own_small_ref, smalls_ref.at[mine], send_s.at[k], recv_s.at[k], device_of(peer, inner)
        )

    def send_small(k, carry):
        small_copy(k).start()
        return carry

    lax.fori_loop(1, count, send_small, 0)
    smalls_ref[mine] = own_small_ref[...]

    total = acc_ref[...] / npw_total
    for k in range(1, inner):
        first_copy(k).wait_recv()
        total += got_ref[lax.rem(me_inner + inner - k, inner)].astype(jnp.float32)
    acc_ref[...] = total
    mid_ref[...] = total.astype(bf)

    def rows_of(place):
        return pl.ds(pl.multiple_of(place * per_outer, per_outer), per_outer)

    def second_copy(k):
        place = to_outer(k)
        return remote(
            mid_ref.at[rows_of(place)], got2_ref.at[me_outer], send2.at[k], recv2.at[k],
            {GROUP[0]: place},
        )

    for k in range(1, outer):
        second_copy(k).start()
    total = acc_ref[rows_of(me_outer), :]
    for k in range(1, outer):
        second_copy(k).wait_recv()
        total += got2_ref[lax.rem(me_outer + outer - k, outer)].astype(jnp.float32)
    all_ref[me_inner, rows_of(me_outer), :] = total.astype(bf)

    own_rows = all_ref.at[me_inner, rows_of(me_outer)]

    def z_copy(k):
        return remote(own_rows, own_rows, send_z.at[k], recv_z.at[k], {GROUP[0]: to_outer(k)})

    def xy_copy(place, step, k):
        ref = all_ref.at[me_inner, rows_of(place)]
        sem = step * inner + k
        return remote(ref, ref, send_xy.at[sem], recv_xy.at[sem], {GROUP[1]: to_inner(k)})

    for k in range(1, outer):
        z_copy(k).start()
    for k in range(1, inner):
        xy_copy(me_outer, 0, k).start()
    for step in range(1, outer):
        z_copy(step).wait_recv()
        place = lax.rem(me_outer + outer - step, outer)
        for k in range(1, inner):
            xy_copy(place, step, k).start()

    width = 4 * lanes

    def project(quarter, first):
        rows = pl.ds(pl.multiple_of(quarter * per_inner, per_inner), per_inner)

        def step(i, carry):
            at = pl.ds(pl.multiple_of(i * width, width), width)
            done = mm(all_ref[quarter], c_ref[rows, at])
            proj_ref[:, at] = done if first else proj_ref[:, at] + done
            return carry

        lax.fori_loop(0, entries // width, step, 0)

    project(me_inner, True)

    def rest(k, carry):
        quarter = lax.rem(me_inner + inner - k, inner)
        for step in range(outer):
            xy_copy(me_outer, step, k).wait_recv()
        project(quarter, False)
        return carry

    lax.fori_loop(1, inner, rest, 0)

    def close(j, carry):
        at = pl.ds(pl.multiple_of(j * lanes, lanes), lanes)
        turned = quarter_turn(proj_ref[BLOCK:, at], -1.0)
        search = pair_ref[:BLOCK, at].astype(jnp.float32)
        out_ref[:, at] = (search - (proj_ref[:BLOCK, at] + turned)).astype(bf)
        return carry

    lax.fori_loop(0, blocks, close, 0)

    for k in range(1, count):
        small_copy(k).wait_recv()
    summed = smalls_ref[0]
    for d in range(1, count):
        summed += smalls_ref[d]
    small_ref[...] = summed

    for k in range(1, count):
        small_copy(k).wait_send()
    for k in range(1, inner):
        first_copy(k).wait_send()
        for step in range(outer):
            xy_copy(me_outer, step, k).wait_send()
    for k in range(1, outer):
        second_copy(k).wait_send()
        z_copy(k).wait_send()


def project_all(flat_all, search, density, ritz, own_pos, strength):
    count, inner, outer = lax.axis_size(GROUP), lax.axis_size(GROUP[1]), lax.axis_size(GROUP[0])
    bands, entries = flat_all.shape
    atoms = own_pos.shape[1]
    two = 2 * BLOCK
    whole = pl.BlockSpec(memory_space=pltpu.VMEM)
    f32, bf = jnp.float32, jnp.bfloat16
    sem = pltpu.SemaphoreType.DMA
    return pl.pallas_call(
        project_kernel,
        in_specs=[whole] * 6,
        out_specs=[whole] * 2,
        out_shape=[
            jax.ShapeDtypeStruct((BLOCK, entries), bf),
            jax.ShapeDtypeStruct((8, atoms), f32),
        ],
        scratch_shapes=[
            pltpu.VMEM((BLOCK * entries // (4 * W), 4 * W), f32),
            pltpu.VMEM((two, entries), bf),
            pltpu.VMEM((inner, two, bands // inner), bf),
            pltpu.VMEM((inner, two, bands // inner), bf),
            pltpu.VMEM((two, bands // inner), bf),
            pltpu.VMEM((outer, two // outer, bands // inner), bf),
            pltpu.VMEM((inner, two, bands // inner), bf),
            pltpu.VMEM((two, entries), f32),
            pltpu.VMEM((two, bands // inner), f32),
            pltpu.VMEM((8, atoms), f32),
            pltpu.VMEM((count, 8, atoms), f32),
            pltpu.VMEM((G, atoms), f32),
            pltpu.VMEM((G, atoms), f32),
            pltpu.VMEM((3, G, atoms), f32),
            sem((inner,)), sem((inner,)), sem((outer,)), sem((outer,)), sem((outer,)), sem((outer,)),
            sem((inner * outer,)), sem((inner * outer,)), sem((count,)), sem((count,)),
        ],
        compiler_params=pltpu.CompilerParams(
            collective_id=1, has_side_effects=True, vmem_limit_bytes=50 * 1024 * 1024
        ),
        cost_estimate=pl.CostEstimate(
            flops=8 * BLOCK * bands * entries, bytes_accessed=16 << 20, transcendentals=0
        ),
        name="project_all",
    )(flat_all, search, density, ritz, own_pos, strength)


def wrap_offset(values):
    return jnp.mod(values + G // 2, G) - G // 2


def gaussians(coords, grid_cells):
    offset = wrap_offset(grid_cells[None, :] - coords[:, None]).astype(jnp.float32)
    return (jnp.exp(-offset * offset / (2.0 * sigma_cells * sigma_cells)), offset)


def atom_tables(own_pos, y_cells):
    grid_cells = jnp.arange(G, dtype=jnp.int32)
    gauss_x, offset_x = gaussians(own_pos[0], grid_cells)
    gauss_y, offset_y = gaussians(own_pos[1], y_cells)
    gauss_z, offset_z = gaussians(own_pos[2], grid_cells)
    return (gauss_x, offset_x, gauss_y, offset_y, gauss_z, offset_z)


def local_potential(tables, strength):
    gauss_x, offset_x, gauss_y, offset_y, gauss_z, offset_z = tables
    atom_count = gauss_x.shape[0]
    joined = (gauss_y[:, :, None] * gauss_z[:, None, :]).reshape(atom_count, -1)
    potential = jnp.dot((strength[:, None] * gauss_x).T, joined, precision=highest)
    return (potential, joined)


def chain_forces(force, own_pos, before, after):
    ahead_step = wrap_offset(after - own_pos).astype(jnp.float32)
    behind = wrap_offset(own_pos - before).astype(jnp.float32)
    tangent_raw = ahead_step + behind
    entries = 3 * own_pos.shape[1]
    tangent = (
        tangent_raw * lax.rsqrt(jnp.mean(tangent_raw * tangent_raw) + epsilon) / math.sqrt(entries)
    )
    length_ahead = jnp.sqrt(entries * (jnp.mean(ahead_step * ahead_step) + epsilon))
    length_behind = jnp.sqrt(entries * (jnp.mean(behind * behind) + epsilon))
    along_path = jnp.sum(force * tangent)
    band_push = (
        force - along_path * tangent + spring_constant * (length_ahead - length_behind) * tangent
    )
    return (band_push, along_path)


def body(coefficients, rotation, positions, start_pos, end_pos, species, depth):
    axes = ("band", "pw")
    devices = lax.axis_size(axes)
    coeff_all = coefficients[0]
    planes = coeff_all.shape[1]
    flat_all = coeff_all.reshape(BANDS, -1)
    vectors = BLOCK // devices
    orbitals = jnp.einsum("ib,ik->bk", rotation[0], flat_all, preferred_element_type=jnp.float32)
    orbitals = orbitals.astype(jnp.bfloat16).reshape(BLOCK, planes * (W // 2), 4 * W)
    orbitals = orbitals.reshape(devices, vectors, planes, W // 2, 4 * W)
    kind_ids = jnp.arange(SPECIES, dtype=jnp.int32)
    strength = jnp.sum(jnp.where(species[:, None] == kind_ids[None, :], depth[None, :], 0.0), 1)
    own_pos = positions[0]
    tables = atom_tables(own_pos, jnp.arange(G, dtype=jnp.int32))
    potential, joined = local_potential(tables, strength)
    potential = jnp.swapaxes(potential.reshape(G, G, G), 0, 1)
    potential = jnp.concatenate([potential, potential], 2)
    search, ritz, density = apply_all(orbitals, potential)
    correction, small = project_all(flat_all, search, density, ritz, own_pos, strength[None])
    ritz_values, atom_force = small[0], small[1:4]
    correction = correction.reshape(BLOCK, planes, W * 2 * W)
    image_idx = lax.axis_index("img")
    before = passed_along(own_pos, "img", 1)
    after = passed_along(own_pos, "img", -1)
    before = jnp.where(image_idx == 0, start_pos, before)
    after = jnp.where(image_idx == lax.axis_size("img") - 1, end_pos, after)
    band_push, along_path = chain_forces(atom_force, own_pos, before, after)
    return (correction[None], ritz_values[None], band_push[None], along_path[None])


def solution(mesh):
    in_specs = (
        P("img", None, ("band", "pw"), None),
        P("img", None, None),
        P("img", None, None),
        P(),
        P(),
        P(),
        P(),
    )
    out_specs = (
        P("img", None, ("band", "pw"), None),
        P("img", None),
        P("img", None, None),
        P("img"),
    )
    return jax.shard_map(body, mesh=mesh, in_specs=in_specs, out_specs=out_specs, check_vma=False)
```

```python
import math

import jax
import jax.numpy as jnp
import numpy as np
from jax import lax
from jax.experimental import pallas as pl
from jax.experimental.pallas import tpu as pltpu
from jax.sharding import PartitionSpec as P

G = 64
W = 32
BANDS = 1024
BLOCK = 256
SPECIES = 4


kinetic_scale = 0.01
sigma_cells = 3.0
spring_constant = 2.0
epsilon = 1e-06


def phases():
    wavenum = np.arange(W, dtype=np.int32) - W // 2
    grid_cells = np.arange(G, dtype=np.int32)
    turn_count = np.mod(wavenum[:, None] * grid_cells[None, :], G)
    return turn_count.astype(np.float32) * np.float32(2.0 * math.pi / G)


def forward_table():
    angle_tab = phases()
    cosine = np.cos(angle_tab) / np.float32(math.sqrt(W))
    sine_part = np.sin(angle_tab) / np.float32(math.sqrt(W))
    return np.stack([np.stack([cosine, sine_part], 1), np.stack([-sine_part, cosine], 1)], 0)


def inverse_table():
    angle_tab = phases().T
    factor = np.float32(math.sqrt(W) / G)
    cosine = np.cos(angle_tab) * factor
    sine_part = np.sin(angle_tab) * factor
    return np.stack([np.stack([cosine, -sine_part], 1), np.stack([sine_part, cosine], 1)], 0)


def kernel_tables():
    fwd = forward_table()
    inv = inverse_table()
    two = np.eye(2, dtype=np.float32)
    table_z = np.einsum("czdn,vw,ij->jviczdwn", fwd, two, two).reshape(2, 8 * W, 4 * G)
    back_z = np.einsum("dncz,vw,ij->jdwnvicz", inv, two, two).reshape(2, 4 * G, 8 * W)
    fwd_y = fwd.reshape(2, W // 2, 2, 2, G)
    table_y = np.einsum("dgpem->empdg", fwd_y).reshape(2 * G, 2 * W)
    table_x = np.einsum("dxem->emxd", fwd).reshape(2 * G, 2 * W)
    back_x = np.einsum("emdx->xdem", inv).reshape(2 * W, 2 * G)
    inv_y = inv.reshape(2, G, 2, W // 2, 2)
    back_y = np.einsum("dmcgp->pcgdm", inv_y).reshape(2 * W, 2 * G)
    listed = (table_z, table_y, table_x, back_x, back_y, back_z)
    return [jnp.asarray(t, dtype=jnp.bfloat16) for t in listed]


def kinetic_table():
    wave = np.arange(W, dtype=np.int32) - W // 2
    sq = wave * wave
    squared = sq[:, None, None, None] + sq[None, :, None, None] + sq[None, None, None, :]
    squared = np.broadcast_to(squared, (W, W, 2, W)).reshape(W * W // 2, 4 * W)
    return np.float32(kinetic_scale * 0.5) * squared.astype(np.float32)


def mm(left, right):
    return jnp.dot(left, right, preferred_element_type=jnp.float32)


MESH_ID = pl.DeviceIdType.MESH
GROUP = ("band", "pw")
X_GROUP = 4
HALVES = 2
SPREAD = G + 8


def group_place():
    inner = lax.axis_size(GROUP[1])
    count = lax.axis_size(GROUP[0]) * inner
    mine = lax.axis_index(GROUP[0]) * inner + lax.axis_index(GROUP[1])
    return mine, count, inner


def device_of(index, inner):
    return {GROUP[0]: index // inner, GROUP[1]: lax.rem(index, inner)}


def greet_all(mine, count, inner, image, images):
    barrier = pltpu.get_barrier_semaphore()
    for k in range(1, count):
        peer = lax.rem(mine + k, count)
        pl.semaphore_signal(
            barrier, inc=1, device_id=device_of(peer, inner), device_id_type=MESH_ID
        )
    beside = sorted({1, images - 1} - {0})
    for step in beside:
        other = lax.rem(image + step, images)
        pl.semaphore_signal(barrier, inc=1, device_id={"img": other}, device_id_type=MESH_ID)
    pl.semaphore_wait(barrier, count - 1 + len(beside))


def atom_rows(pos_ref, axis):
    cell = lax.broadcasted_iota(jnp.int32, (G, pos_ref.shape[1]), 0)
    shifted = (cell - pos_ref[axis : axis + 1, :] + G // 2) & (G - 1)
    offset = (shifted - G // 2).astype(jnp.float32)
    return jnp.exp(-offset * offset / (2.0 * sigma_cells * sigma_cells)), offset


def split_two(values):
    high = values.astype(jnp.bfloat16)
    return high, (values - high.astype(jnp.float32)).astype(jnp.bfloat16)


def fill_potential(pos_ref, strength_ref, gy_ref, pot_ref):
    gauss_x = atom_rows(pos_ref, 0)[0] * strength_ref[...]
    gy_ref[...] = atom_rows(pos_ref, 1)[0]
    gauss_z = atom_rows(pos_ref, 2)[0]
    high, low = split_two(jnp.transpose(jnp.concatenate([gauss_z, gauss_z], axis=0)))
    table = jnp.concatenate([high, low], axis=1)
    group = 4

    def step(i, carry):
        rows = []
        for k in range(group):
            rows.extend(split_two(gauss_x * gy_ref[pl.ds(group * i + k, 1), :]))
        done = mm(jnp.concatenate(rows, axis=0), table)
        for k in range(group):
            top = done[2 * k * G : (2 * k + 1) * G]
            rest = done[(2 * k + 1) * G : (2 * k + 2) * G]
            pot_ref[group * i + k] = top[:, : 2 * G] + (top[:, 2 * G :] + rest[:, : 2 * G])
        return carry

    lax.fori_loop(0, G // group, step, 0)


def quarter_turn(values, sign):
    lane = lax.broadcasted_iota(jnp.int32, values.shape, 1)
    first = (lane // W) % 2 == 0
    size = values.shape[1]
    later = pltpu.roll(values, size - W, 1)
    earlier = pltpu.roll(values, W, 1)
    return jnp.where(first, sign * later, -sign * earlier)


def partial_forces(dens_ref, pos_ref, strength_ref, gy_ref, gyd_ref, f_ref):
    atoms = pos_ref.shape[1]
    gauss_x, offset_x = atom_rows(pos_ref, 0)
    gauss_y, offset_y = atom_rows(pos_ref, 1)
    gauss_z, offset_z = atom_rows(pos_ref, 2)
    gy_ref[...] = gauss_y
    gyd_ref[...] = gauss_y * offset_y
    high, low = split_two(jnp.concatenate([gauss_z, gauss_z * offset_z], axis=1))
    table = jnp.concatenate([high, high, low, jnp.zeros_like(low)], axis=0)
    f_ref[...] = jnp.zeros_like(f_ref)
    group = 4
    left = lax.broadcasted_iota(jnp.int32, (G, 2 * G), 1) < G

    def step(i, carry):
        rows = []
        for k in range(group):
            pair = dens_ref[group * i + k]
            both = (pair + pltpu.roll(pair, G, 1)) * (1.0 / BLOCK)
            high_part = both.astype(jnp.bfloat16).astype(jnp.float32)
            rest = both - high_part
            rows.append(
                jnp.concatenate(
                    [jnp.where(left, high_part, rest), jnp.where(left, high_part, 0.0)], axis=1
                ).astype(jnp.bfloat16)
            )
        done = mm(jnp.concatenate(rows, axis=0), table)
        sums = [f_ref[m] for m in range(3)]
        for k in range(group):
            plain = done[k * G : (k + 1) * G, :atoms]
            along = done[k * G : (k + 1) * G, atoms:]
            at = pl.ds(group * i + k, 1)
            gauss = gy_ref[at, :]
            sums[0] += gauss * plain
            sums[1] += gyd_ref[at, :] * plain
            sums[2] += gauss * along
        for m in range(3):
            f_ref[m] = sums[m]
        return carry

    lax.fori_loop(0, G // group, step, 0)
    prefactor = -strength_ref[...] / (sigma_cells * sigma_cells)
    weights = [gauss_x * offset_x, gauss_x, gauss_x]
    return [prefactor * jnp.sum(weights[m] * f_ref[m], axis=0, keepdims=True) for m in range(3)]


def wrap_offset(values):
    return ((values + G // 2) & (G - 1)) - G // 2


def chain_forces(force, own_pos, before, after):
    ahead_step = wrap_offset(after - own_pos).astype(jnp.float32)
    behind = wrap_offset(own_pos - before).astype(jnp.float32)
    tangent_raw = ahead_step + behind
    entries = own_pos.size

    def total(values):
        return jnp.sum(jnp.sum(values, axis=0, keepdims=True), axis=1, keepdims=True)

    def mean_square(values):
        return total(values * values) * (1.0 / entries)

    tangent = tangent_raw * (
        lax.rsqrt(mean_square(tangent_raw) + epsilon) * (1.0 / math.sqrt(entries))
    )
    length_ahead = jnp.sqrt(entries * (mean_square(ahead_step) + epsilon))
    length_behind = jnp.sqrt(entries * (mean_square(behind) + epsilon))
    along_path = total(force * tangent)
    push = spring_constant * (length_ahead - length_behind) - along_path
    return force + push * tangent, along_path


def step_kernel(
    c_hbm, orb_ref, pos_ref, strength_ref, start_ref, end_ref,
    kin_ref, tz_ref, ty_ref, tx_ref, bx_ref, by_ref, bz_ref,
    out_ref, small_ref,
    c_ref, in_ref, back_ref, search_ref, zs_ref, s_ref, pot_ref, dens_ref, gy_ref, gyd_ref, f_ref,
    wide_ref, pair_ref, part_ref, got_ref, mid_ref, got2_ref, all_ref, proj_ref, acc_ref,
    own_small_ref, smalls_ref, near_ref,
    load_sem, send_sem, recv_sem, back_send_sem, back_recv_sem,
    send1, recv1, send2, recv2, send_z, recv_z, send_xy, recv_xy, send_s, recv_s, send_n, recv_n,
):
    lanes = 2 * G
    half = W // 2
    rows = W * half
    bf = jnp.bfloat16
    mine, count, inner = group_place()
    chunks = orb_ref.shape[1] // 2

    images = lax.axis_size("img")
    image = lax.axis_index("img")
    load_c = pltpu.make_async_copy(c_hbm, c_ref, load_sem.at[0])
    load_c.start()

    def near_copy(side):
        other = lax.rem(image + (1, images - 1)[side], images)
        return pltpu.make_async_remote_copy(
            src_ref=pos_ref, dst_ref=near_ref.at[side], send_sem=send_n.at[side],
            recv_sem=recv_n.at[side], device_id={"img": other}, device_id_type=MESH_ID,
        )

    greet_all(mine, count, inner, image, images)
    if images > 1:
        for side in range(2):
            near_copy(side).start()

    def send_chunk(c, carry):
        at = pl.ds(2 * c, 2)
        for k in range(1, count):
            peer = lax.rem(mine + k, count)
            pltpu.make_async_remote_copy(
                src_ref=orb_ref.at[peer, at],
                dst_ref=in_ref.at[mine, at],
                send_sem=send_sem.at[c],
                recv_sem=recv_sem.at[c],
                device_id=device_of(peer, inner),
                device_id_type=MESH_ID,
            ).start()
        return carry

    lax.fori_loop(0, chunks, send_chunk, 0)
    in_ref[mine] = orb_ref[mine]
    dens_ref[...] = jnp.zeros_like(dens_ref)
    own_small_ref[...] = jnp.zeros_like(own_small_ref)
    fill_potential(pos_ref, strength_ref, gy_ref, pot_ref)

    def all_of(ref, c, sem):
        part = ref.at[pl.ds(0, count - 1), pl.ds(2 * c, 2)]
        return pltpu.make_async_copy(part, part, sem.at[c])

    def chunk_step(c, chunk_carry):
        all_of(in_ref, c, recv_sem).wait()
        vecs = jnp.concatenate(
            [in_ref[:, 2 * c + v].reshape(rows, 4 * W) for v in range(2)], axis=1
        )
        for p in range(2):
            zs_ref[p] = mm(vecs, tz_ref[p]).astype(bf)

        def y_step(i, carry):
            cols = []
            for k in range(2):
                at = pl.ds(pl.multiple_of((2 * i + k) * half, half), half)
                parts = [
                    zs_ref[p, at, d * lanes : (d + 1) * lanes] for p in range(2) for d in range(2)
                ]
                cols.append(jnp.concatenate(parts, axis=0))
            done = mm(ty_ref[...], jnp.concatenate(cols, axis=1))
            for k in range(2):
                for e in range(2):
                    start = pl.multiple_of((4 * i + 2 * k + e) * SPREAD, 8)
                    s_ref[pl.ds(start, G), :] = done[
                        e * G : (e + 1) * G, k * lanes : (k + 1) * lanes
                    ]
            return carry

        lax.fori_loop(0, W // 2, y_step, 0, unroll=4)

        def x_step(i, carry):
            first = 2 * X_GROUP * i
            ats = [pl.ds(first + k, 2 * W, stride=SPREAD) for k in range(2 * X_GROUP)]
            cols = [s_ref[at, :].astype(bf) for at in ats]
            for u in range(X_GROUP):
                done = mm(tx_ref[...], jnp.concatenate(cols[2 * u : 2 * u + 2], axis=1))
                real, imag = (done[:G], done[G:])
                pot = jnp.concatenate(
                    [pot_ref[first + 2 * u], pot_ref[first + 2 * u + 1]], axis=1
                )
                square = real * real + imag * imag
                for k in range(2):
                    dens_ref[first + 2 * u + k] += square[:, k * lanes : (k + 1) * lanes]
                weighted = jnp.concatenate(
                    [(real * pot).astype(bf), (imag * pot).astype(bf)], axis=0
                )
                back = mm(bx_ref[...], weighted)
                for k in range(2):
                    s_ref[ats[2 * u + k], :] = back[:, k * lanes : (k + 1) * lanes]
            return carry

        lax.fori_loop(0, G // (2 * X_GROUP), x_step, 0)

        def back_y_step(i, carry):
            cols = []
            for k in range(2):
                parts = []
                for e in range(2):
                    start = pl.multiple_of((4 * i + 2 * k + e) * SPREAD, 8)
                    parts.append(s_ref[pl.ds(start, G), :])
                cols.append(jnp.concatenate(parts, axis=0).astype(bf))
            done = mm(by_ref[...], jnp.concatenate(cols, axis=1)).astype(bf)
            for k in range(2):
                at = pl.ds(pl.multiple_of((2 * i + k) * half, half), half)
                for p in range(2):
                    for q in range(2):
                        r = (2 * p + q) * half
                        zs_ref[p, at, q * lanes : (q + 1) * lanes] = done[
                            r : r + half, k * lanes : (k + 1) * lanes
                        ]
            return carry

        lax.fori_loop(0, W // 2, back_y_step, 0, unroll=4)

        local = mm(zs_ref[0], bz_ref[0]) + mm(zs_ref[1], bz_ref[1])
        kin = kin_ref[...]
        npw_total = W * W * W
        for v in range(2):
            orb = in_ref[:, 2 * c + v].reshape(rows, 4 * W).astype(jnp.float32)
            ham = kin * orb + local[:, v * 4 * W : (v + 1) * 4 * W]
            numerator = jnp.sum(jnp.sum(orb * ham, axis=0, keepdims=True), axis=1, keepdims=True)
            denominator = jnp.sum(jnp.sum(orb * orb, axis=0, keepdims=True), axis=1, keepdims=True)
            ritz = numerator / npw_total / (denominator / npw_total + epsilon)
            search = ((ham - ritz * orb) / (1.0 + kin)).astype(bf)
            back_ref[:, 2 * c + v] = search.reshape(in_ref.shape[0], *in_ref.shape[2:])
            slot = lax.broadcasted_iota(jnp.int32, own_small_ref.shape, 1)
            here = slot == mine * orb_ref.shape[1] + 2 * c + v
            own_small_ref[...] = jnp.where(here, ritz, own_small_ref[...])
        at = pl.ds(2 * c, 2)
        search_ref[mine, at] = back_ref[mine, at]
        for k in range(1, count):
            peer = lax.rem(mine + k, count)
            pltpu.make_async_remote_copy(
                src_ref=back_ref.at[peer, at],
                dst_ref=search_ref.at[mine, at],
                send_sem=back_send_sem.at[c],
                recv_sem=back_recv_sem.at[c],
                device_id=device_of(peer, inner),
                device_id_type=MESH_ID,
            ).start()
        return chunk_carry

    lax.fori_loop(0, chunks, chunk_step, 0)

    outer = count // inner
    me_outer, me_inner = lax.axis_index(GROUP[0]), lax.axis_index(GROUP[1])
    bands, entries = c_ref.shape
    wide_lanes = 4 * W
    blocks = entries // wide_lanes
    per_inner = bands // inner
    each = orb_ref.shape[1] // HALVES
    vecs_half = BLOCK // HALVES
    two = 2 * vecs_half
    per_outer = two // outer
    spread = blocks + 8
    npw_total = W * W * W
    depth = entries // 4

    def remote(src, dst, send, recv, where):
        return pltpu.make_async_remote_copy(
            src_ref=src, dst_ref=dst, send_sem=send, recv_sem=recv,
            device_id=where, device_id_type=MESH_ID,
        )

    def to_inner(k):
        return lax.rem(me_inner + k, inner)

    def to_outer(k):
        return lax.rem(me_outer + k, outer)

    def rows_of(place):
        return pl.ds(pl.multiple_of(place * per_outer, per_outer), per_outer)

    def arrange(h):
        def wait_chunk(c, carry):
            all_of(search_ref, c, back_recv_sem).wait()
            return carry

        share = chunks // HALVES
        lax.fori_loop(h * share, (h + 1) * share, wait_chunk, 0)

        def widen(i, carry):
            for v in range(each):
                at = pl.ds(pl.multiple_of((i * each + v) * spread, 8), blocks)
                values = search_ref[i, h * each + v].reshape(blocks, wide_lanes)
                wide_ref[at, :] = values.astype(jnp.float32)
            return carry

        lax.fori_loop(0, count, widen, 0)

        def lay(j, carry):
            block = wide_ref[pl.ds(j, vecs_half, stride=spread), :]
            at = pl.ds(pl.multiple_of(j * wide_lanes, wide_lanes), wide_lanes)
            pair_ref[h, :vecs_half, at] = block.astype(bf)
            pair_ref[h, vecs_half:, at] = quarter_turn(block, 1.0).astype(bf)
            return carry

        lax.fori_loop(0, blocks, lay, 0)

    def overlap(h, quarter):
        rows = pl.ds(pl.multiple_of(quarter * per_inner, per_inner), per_inner)
        acc_ref[h] = jnp.zeros(acc_ref.shape[1:], jnp.float32)

        def step(i, carry):
            at = pl.ds(pl.multiple_of(i * depth, depth), depth)
            acc_ref[h] += lax.dot_general(
                pair_ref[h, :, at], c_ref[rows, at], (((1,), (1,)), ((), ())),
                preferred_element_type=jnp.float32,
            )
            return carry

        lax.fori_loop(0, entries // depth, step, 0)

    def first_copy(h, k):
        quarter, sem = to_inner(k), h * inner + k
        return remote(
            part_ref.at[h, quarter], got_ref.at[h, me_inner], send1.at[sem], recv1.at[sem],
            {GROUP[1]: quarter},
        )

    def overlap_all(h):
        def send_quarter(k, carry):
            quarter = to_inner(k)
            overlap(h, quarter)
            part_ref[h, quarter] = (acc_ref[h] / npw_total).astype(bf)
            first_copy(h, k).start()
            return carry

        lax.fori_loop(1, inner, send_quarter, 0)
        overlap(h, me_inner)

    def second_copy(h, k):
        place, sem = to_outer(k), h * outer + k
        return remote(
            mid_ref.at[h, rows_of(place)], got2_ref.at[h, me_outer], send2.at[sem], recv2.at[sem],
            {GROUP[0]: place},
        )

    def second_stage(h):
        total = acc_ref[h] / npw_total
        for k in range(1, inner):
            first_copy(h, k).wait_recv()
            total += got_ref[h, lax.rem(me_inner + inner - k, inner)].astype(jnp.float32)
        acc_ref[h] = total
        mid_ref[h] = total.astype(bf)
        for k in range(1, outer):
            second_copy(h, k).start()

    def z_copy(h, k):
        ref = all_ref.at[h, me_inner, rows_of(me_outer)]
        sem = h * outer + k
        return remote(ref, ref, send_z.at[sem], recv_z.at[sem], {GROUP[0]: to_outer(k)})

    def xy_copy(h, place, step, k):
        ref = all_ref.at[h, me_inner, rows_of(place)]
        sem = (h * outer + step) * inner + k
        return remote(ref, ref, send_xy.at[sem], recv_xy.at[sem], {GROUP[1]: to_inner(k)})

    def third_stage(h):
        total = acc_ref[h, rows_of(me_outer), :]
        for k in range(1, outer):
            second_copy(h, k).wait_recv()
            total += got2_ref[h, lax.rem(me_outer + outer - k, outer)].astype(jnp.float32)
        all_ref[h, me_inner, rows_of(me_outer), :] = total.astype(bf)
        for k in range(1, outer):
            z_copy(h, k).start()
        for k in range(1, inner):
            xy_copy(h, me_outer, 0, k).start()

    def forward(h):
        for step in range(1, outer):
            z_copy(h, step).wait_recv()
            place = lax.rem(me_outer + outer - step, outer)
            for k in range(1, inner):
                xy_copy(h, place, step, k).start()

    width = 4 * wide_lanes

    def project(h, quarter, first):
        rows = pl.ds(pl.multiple_of(quarter * per_inner, per_inner), per_inner)

        def step(i, carry):
            at = pl.ds(pl.multiple_of(i * width, width), width)
            done = mm(all_ref[h, quarter], c_ref[rows, at])
            proj_ref[h, :, at] = done if first else proj_ref[h, :, at] + done
            return carry

        lax.fori_loop(0, entries // width, step, 0)

    def project_rest(h):
        def rest(k, carry):
            for step in range(outer):
                xy_copy(h, me_outer, step, k).wait_recv()
            project(h, lax.rem(me_inner + inner - k, inner), False)
            return carry

        lax.fori_loop(1, inner, rest, 0)

    def small_copy(k):
        peer = lax.rem(mine + k, count)
        return remote(
            own_small_ref, smalls_ref.at[mine], send_s.at[k], recv_s.at[k], device_of(peer, inner)
        )

    def send_small(k, carry):
        small_copy(k).start()
        return carry

    load_c.wait()
    arrange(0)
    overlap_all(0)
    arrange(1)
    second_stage(0)
    overlap_all(1)
    third_stage(0)

    forces = partial_forces(dens_ref, pos_ref, strength_ref, gy_ref, gyd_ref, f_ref)
    for m in range(3):
        own_small_ref[m : m + 1, :] = forces[m]
    lax.fori_loop(1, count, send_small, 0)
    smalls_ref[mine] = own_small_ref[...]

    second_stage(1)
    forward(0)
    project(0, me_inner, True)
    third_stage(1)
    project_rest(0)
    forward(1)
    project(1, me_inner, True)

    for k in range(1, count):
        small_copy(k).wait_recv()
    summed = smalls_ref[0]
    for d in range(1, count):
        summed += smalls_ref[d]
    own = pos_ref[...]
    if images > 1:
        for side in range(2):
            near_copy(side).wait_recv()
        before = jnp.where(image == 0, start_ref[...], near_ref[0])
        after = jnp.where(image == images - 1, end_ref[...], near_ref[1])
    else:
        before, after = start_ref[...], end_ref[...]
    band, along = chain_forces(summed[:3], own, before, after)
    small_ref[...] = summed
    small_ref[:3] = band
    small_ref[4:5] = jnp.broadcast_to(along, (1, small_ref.shape[1]))

    project_rest(1)

    def close(j, carry):
        at = pl.ds(pl.multiple_of(j * wide_lanes, wide_lanes), wide_lanes)
        parts = []
        for h in range(HALVES):
            turned = quarter_turn(proj_ref[h, vecs_half:, at], -1.0)
            search = pair_ref[h, :vecs_half, at].astype(jnp.float32)
            left = search - (proj_ref[h, :vecs_half, at] + turned)
            parts.append(left.reshape(count, 1, each, wide_lanes))
        joined = jnp.concatenate(parts, axis=1).reshape(BLOCK, wide_lanes)
        out_ref[:, at] = joined.astype(bf)
        return carry

    lax.fori_loop(0, blocks, close, 0)

    def finish(c, carry):
        all_of(in_ref, c, send_sem).wait()
        all_of(search_ref, c, back_send_sem).wait()
        return carry

    lax.fori_loop(0, chunks, finish, 0)
    for k in range(1, count):
        small_copy(k).wait_send()
    for h in range(HALVES):
        for k in range(1, inner):
            first_copy(h, k).wait_send()
            for step in range(outer):
                xy_copy(h, me_outer, step, k).wait_send()
        for k in range(1, outer):
            second_copy(h, k).wait_send()
            z_copy(h, k).wait_send()
    if images > 1:
        for side in range(2):
            near_copy(side).wait_send()


def whole_step(flat_all, orbitals, own_pos, strength, start_pos, end_pos):
    devices, vectors, planes, half, lanes = orbitals.shape
    inner, outer = lax.axis_size(GROUP[1]), lax.axis_size(GROUP[0])
    bands, entries = flat_all.shape
    atoms = own_pos.shape[1]
    tabs = kernel_tables()
    kin = jnp.asarray(kinetic_table())
    whole = pl.BlockSpec(memory_space=pltpu.VMEM)
    chunks = vectors // 2
    f32, bf = jnp.float32, jnp.bfloat16
    sem, vmem = pltpu.SemaphoreType.DMA, pltpu.VMEM
    two = 2 * BLOCK // HALVES
    share = bands // inner
    flops = vectors * 2 * 2 * (W * W * 2 * W * 2 * G + W * G * 2 * W * 2 * G + G * G * 2 * W * 2 * G)
    flops += 8 * BLOCK * bands * entries
    return pl.pallas_call(
        step_kernel,
        in_specs=[pl.BlockSpec(memory_space=pltpu.HBM)] + [whole] * 12,
        out_specs=[whole] * 2,
        out_shape=[
            jax.ShapeDtypeStruct((BLOCK, entries), bf),
            jax.ShapeDtypeStruct((8, atoms), f32),
        ],
        scratch_shapes=[
            vmem((bands, entries), bf),
            vmem(orbitals.shape, bf),
            vmem(orbitals.shape, bf),
            vmem(orbitals.shape, bf),
            vmem((2, W * W // 2, 4 * G), bf),
            vmem((2 * W * SPREAD, 2 * G), f32),
            vmem((G, G, 2 * G), f32),
            vmem((G, G, 2 * G), f32),
            vmem((G, atoms), f32),
            vmem((G, atoms), f32),
            vmem((3, G, atoms), f32),
            vmem((BLOCK // HALVES * (entries // (4 * W) + 8), 4 * W), f32),
            vmem((HALVES, two, entries), bf),
            vmem((HALVES, inner, two, share), bf),
            vmem((HALVES, inner, two, share), bf),
            vmem((HALVES, two, share), bf),
            vmem((HALVES, outer, two // outer, share), bf),
            vmem((HALVES, inner, two, share), bf),
            vmem((HALVES, two, entries), f32),
            vmem((HALVES, two, share), f32),
            vmem((8, atoms), f32),
            vmem((devices, 8, atoms), f32),
            vmem((2, 3, atoms), jnp.int32),
            sem((1,)), sem((chunks,)), sem((chunks,)), sem((chunks,)), sem((chunks,)),
            sem((HALVES * inner,)), sem((HALVES * inner,)),
            sem((HALVES * outer,)), sem((HALVES * outer,)),
            sem((HALVES * outer,)), sem((HALVES * outer,)),
            sem((HALVES * inner * outer,)), sem((HALVES * inner * outer,)),
            sem((devices,)), sem((devices,)), sem((2,)), sem((2,)),
        ],
        compiler_params=pltpu.CompilerParams(
            collective_id=0, has_side_effects=True, vmem_limit_bytes=62 * 1024 * 1024
        ),
        cost_estimate=pl.CostEstimate(flops=flops, bytes_accessed=16 << 20, transcendentals=0),
        name="whole_step",
    )(flat_all, orbitals, own_pos, strength, start_pos, end_pos, kin, *tabs)


def body(coefficients, rotation, positions, start_pos, end_pos, species, depth):
    devices = lax.axis_size(GROUP)
    coeff_all = coefficients[0]
    planes = coeff_all.shape[1]
    flat_all = coeff_all.reshape(BANDS, -1)
    vectors = BLOCK // devices
    orbitals = jnp.einsum("ib,ik->bk", rotation[0], flat_all, preferred_element_type=jnp.float32)
    orbitals = orbitals.astype(jnp.bfloat16)
    orbitals = orbitals.reshape(devices, vectors, planes, W // 2, 4 * W)
    kind_ids = jnp.arange(SPECIES, dtype=jnp.int32)
    strength = jnp.sum(jnp.where(species[:, None] == kind_ids[None, :], depth[None, :], 0.0), 1)
    strength = strength[None]
    own_pos = positions[0]
    correction, small = whole_step(flat_all, orbitals, own_pos, strength, start_pos, end_pos)
    correction = correction.reshape(BLOCK, planes, W * 2 * W)
    return (correction[None], small[3:4], small[None, :3], small[4, :1])


def solution(mesh):
    in_specs = (
        P("img", None, ("band", "pw"), None),
        P("img", None, None),
        P("img", None, None),
        P(),
        P(),
        P(),
        P(),
    )
    out_specs = (
        P("img", None, ("band", "pw"), None),
        P("img", None),
        P("img", None, None),
        P("img"),
    )
    return jax.shard_map(body, mesh=mesh, in_specs=in_specs, out_specs=out_specs, check_vma=False)
```

```python
import math

import jax
import jax.numpy as jnp
import numpy as np
from jax import lax
from jax.experimental import pallas as pl
from jax.experimental.pallas import tpu as pltpu
from jax.sharding import PartitionSpec as P

G = 64
W = 32
BANDS = 1024
BLOCK = 256
SPECIES = 4


kinetic_scale = 0.01
sigma_cells = 3.0
spring_constant = 2.0
epsilon = 1e-06


def phases():
    wavenum = np.arange(W, dtype=np.int32) - W // 2
    grid_cells = np.arange(G, dtype=np.int32)
    turn_count = np.mod(wavenum[:, None] * grid_cells[None, :], G)
    return turn_count.astype(np.float32) * np.float32(2.0 * math.pi / G)


def forward_table():
    angle_tab = phases()
    cosine = np.cos(angle_tab) / np.float32(math.sqrt(W))
    sine_part = np.sin(angle_tab) / np.float32(math.sqrt(W))
    return np.stack([np.stack([cosine, sine_part], 1), np.stack([-sine_part, cosine], 1)], 0)


def inverse_table():
    angle_tab = phases().T
    factor = np.float32(math.sqrt(W) / G)
    cosine = np.cos(angle_tab) * factor
    sine_part = np.sin(angle_tab) * factor
    return np.stack([np.stack([cosine, -sine_part], 1), np.stack([sine_part, cosine], 1)], 0)


def kernel_tables():
    fwd = forward_table()
    inv = inverse_table()
    two = np.eye(2, dtype=np.float32)
    table_z = np.einsum("czdn,vw,ij->jviczdwn", fwd, two, two).reshape(2, 8 * W, 4 * G)
    back_z = np.einsum("dncz,vw,ij->jdwnvicz", inv, two, two).reshape(2, 4 * G, 8 * W)
    fwd_y = fwd.reshape(2, W // 2, 2, 2, G)
    table_y = np.einsum("dgpem->empdg", fwd_y).reshape(2 * G, 2 * W)
    table_x = np.einsum("dxem->emxd", fwd).reshape(2 * G, 2 * W)
    back_x = np.einsum("emdx->xdem", inv).reshape(2 * W, 2 * G)
    inv_y = inv.reshape(2, G, 2, W // 2, 2)
    back_y = np.einsum("dmcgp->pcgdm", inv_y).reshape(2 * W, 2 * G)
    listed = (table_z, table_y, table_x, back_x, back_y, back_z)
    return [jnp.asarray(t, dtype=jnp.bfloat16) for t in listed]


def kinetic_table():
    wave = np.arange(W, dtype=np.int32) - W // 2
    sq = wave * wave
    squared = sq[:, None, None, None] + sq[None, :, None, None] + sq[None, None, None, :]
    squared = np.broadcast_to(squared, (W, W, 2, W)).reshape(W * W // 2, 4 * W)
    return np.float32(kinetic_scale * 0.5) * squared.astype(np.float32)


def mm(left, right):
    return jnp.dot(left, right, preferred_element_type=jnp.float32)


MESH_ID = pl.DeviceIdType.MESH
GROUP = ("band", "pw")
X_GROUP = 4
HALVES = 2
SPREAD = G + 8


def group_place():
    inner = lax.axis_size(GROUP[1])
    count = lax.axis_size(GROUP[0]) * inner
    mine = lax.axis_index(GROUP[0]) * inner + lax.axis_index(GROUP[1])
    return mine, count, inner


def device_of(index, inner):
    return {GROUP[0]: index // inner, GROUP[1]: lax.rem(index, inner)}


def greet_all(mine, count, inner, image, images):
    barrier = pltpu.get_barrier_semaphore()
    for k in range(1, count):
        peer = lax.rem(mine + k, count)
        pl.semaphore_signal(
            barrier, inc=1, device_id=device_of(peer, inner), device_id_type=MESH_ID
        )
    beside = sorted({1, images - 1} - {0})
    for step in beside:
        other = lax.rem(image + step, images)
        pl.semaphore_signal(barrier, inc=1, device_id={"img": other}, device_id_type=MESH_ID)
    pl.semaphore_wait(barrier, count - 1 + len(beside))


def atom_rows(pos_ref, axis):
    cell = lax.broadcasted_iota(jnp.int32, (G, pos_ref.shape[1]), 0)
    shifted = (cell - pos_ref[axis : axis + 1, :] + G // 2) & (G - 1)
    offset = (shifted - G // 2).astype(jnp.float32)
    return jnp.exp(-offset * offset / (2.0 * sigma_cells * sigma_cells)), offset


def split_two(values):
    high = values.astype(jnp.bfloat16)
    return high, (values - high.astype(jnp.float32)).astype(jnp.bfloat16)


def fill_potential(pos_ref, strength_ref, gy_ref, pot_ref):
    gauss_x = atom_rows(pos_ref, 0)[0] * strength_ref[...]
    gy_ref[...] = atom_rows(pos_ref, 1)[0]
    gauss_z = atom_rows(pos_ref, 2)[0]
    high, low = split_two(jnp.transpose(jnp.concatenate([gauss_z, gauss_z], axis=0)))
    table = jnp.concatenate([high, low], axis=1)
    group = 4

    def step(i, carry):
        rows = []
        for k in range(group):
            rows.extend(split_two(gauss_x * gy_ref[pl.ds(group * i + k, 1), :]))
        done = mm(jnp.concatenate(rows, axis=0), table)
        for k in range(group):
            top = done[2 * k * G : (2 * k + 1) * G]
            rest = done[(2 * k + 1) * G : (2 * k + 2) * G]
            pot_ref[group * i + k] = top[:, : 2 * G] + (top[:, 2 * G :] + rest[:, : 2 * G])
        return carry

    lax.fori_loop(0, G // group, step, 0)


def quarter_turn(values, sign):
    lane = lax.broadcasted_iota(jnp.int32, values.shape, 1)
    first = (lane // W) % 2 == 0
    size = values.shape[1]
    later = pltpu.roll(values, size - W, 1)
    earlier = pltpu.roll(values, W, 1)
    return jnp.where(first, sign * later, -sign * earlier)


def partial_forces(dens_ref, pos_ref, strength_ref, gy_ref, gyd_ref, f_ref):
    atoms = pos_ref.shape[1]
    gauss_x, offset_x = atom_rows(pos_ref, 0)
    gauss_y, offset_y = atom_rows(pos_ref, 1)
    gauss_z, offset_z = atom_rows(pos_ref, 2)
    gy_ref[...] = gauss_y
    gyd_ref[...] = gauss_y * offset_y
    high, low = split_two(jnp.concatenate([gauss_z, gauss_z * offset_z], axis=1))
    table = jnp.concatenate([high, high, low, jnp.zeros_like(low)], axis=0)
    f_ref[...] = jnp.zeros_like(f_ref)
    group = 4
    left = lax.broadcasted_iota(jnp.int32, (G, 2 * G), 1) < G

    def step(i, carry):
        rows = []
        for k in range(group):
            pair = dens_ref[group * i + k]
            both = (pair + pltpu.roll(pair, G, 1)) * (1.0 / BLOCK)
            high_part = both.astype(jnp.bfloat16).astype(jnp.float32)
            rest = both - high_part
            rows.append(
                jnp.concatenate(
                    [jnp.where(left, high_part, rest), jnp.where(left, high_part, 0.0)], axis=1
                ).astype(jnp.bfloat16)
            )
        done = mm(jnp.concatenate(rows, axis=0), table)
        sums = [f_ref[m] for m in range(3)]
        for k in range(group):
            plain = done[k * G : (k + 1) * G, :atoms]
            along = done[k * G : (k + 1) * G, atoms:]
            at = pl.ds(group * i + k, 1)
            gauss = gy_ref[at, :]
            sums[0] += gauss * plain
            sums[1] += gyd_ref[at, :] * plain
            sums[2] += gauss * along
        for m in range(3):
            f_ref[m] = sums[m]
        return carry

    lax.fori_loop(0, G // group, step, 0)
    prefactor = -strength_ref[...] / (sigma_cells * sigma_cells)
    weights = [gauss_x * offset_x, gauss_x, gauss_x]
    return [prefactor * jnp.sum(weights[m] * f_ref[m], axis=0, keepdims=True) for m in range(3)]


def wrap_offset(values):
    return ((values + G // 2) & (G - 1)) - G // 2


def chain_forces(force, own_pos, before, after):
    ahead_step = wrap_offset(after - own_pos).astype(jnp.float32)
    behind = wrap_offset(own_pos - before).astype(jnp.float32)
    tangent_raw = ahead_step + behind
    entries = own_pos.size

    def total(values):
        return jnp.sum(jnp.sum(values, axis=0, keepdims=True), axis=1, keepdims=True)

    def mean_square(values):
        return total(values * values) * (1.0 / entries)

    tangent = tangent_raw * (
        lax.rsqrt(mean_square(tangent_raw) + epsilon) * (1.0 / math.sqrt(entries))
    )
    length_ahead = jnp.sqrt(entries * (mean_square(ahead_step) + epsilon))
    length_behind = jnp.sqrt(entries * (mean_square(behind) + epsilon))
    along_path = total(force * tangent)
    push = spring_constant * (length_ahead - length_behind) - along_path
    return force + push * tangent, along_path


def step_kernel(
    c_hbm, orb_ref, pos_ref, strength_ref, start_ref, end_ref,
    kin_ref, tz_ref, ty_ref, tx_ref, bx_ref, by_ref, bz_ref,
    out_ref, small_ref,
    c_ref, in_ref, back_ref, search_ref, zs_ref, s_ref, pot_ref, dens_ref, gy_ref, gyd_ref, f_ref,
    wide_ref, pair_ref, part_ref, got_ref, mid_ref, got2_ref, all_ref, proj_ref, acc_ref,
    own_small_ref, smalls_ref, near_ref,
    load_sem, send_sem, recv_sem, back_send_sem, back_recv_sem,
    send1, recv1, send2, recv2, send_z, recv_z, send_xy, recv_xy, send_s, recv_s, send_n, recv_n,
):
    lanes = 2 * G
    half = W // 2
    rows = W * half
    bf = jnp.bfloat16
    mine, count, inner = group_place()
    chunks = orb_ref.shape[1] // 2

    images = lax.axis_size("img")
    image = lax.axis_index("img")
    load_c = pltpu.make_async_copy(c_hbm, c_ref, load_sem.at[0])
    load_c.start()

    def near_copy(side):
        other = lax.rem(image + (1, images - 1)[side], images)
        return pltpu.make_async_remote_copy(
            src_ref=pos_ref, dst_ref=near_ref.at[side], send_sem=send_n.at[side],
            recv_sem=recv_n.at[side], device_id={"img": other}, device_id_type=MESH_ID,
        )

    greet_all(mine, count, inner, image, images)
    if images > 1:
        for side in range(2):
            near_copy(side).start()

    def send_chunk(c, carry):
        at = pl.ds(2 * c, 2)
        for k in range(1, count):
            peer = lax.rem(mine + k, count)
            pltpu.make_async_remote_copy(
                src_ref=orb_ref.at[peer, at],
                dst_ref=in_ref.at[mine, at],
                send_sem=send_sem.at[c],
                recv_sem=recv_sem.at[c],
                device_id=device_of(peer, inner),
                device_id_type=MESH_ID,
            ).start()
        return carry

    lax.fori_loop(0, chunks, send_chunk, 0)
    in_ref[mine] = orb_ref[mine]
    dens_ref[...] = jnp.zeros_like(dens_ref)
    own_small_ref[...] = jnp.zeros_like(own_small_ref)
    fill_potential(pos_ref, strength_ref, gy_ref, pot_ref)

    def all_of(ref, c, sem):
        part = ref.at[pl.ds(0, count - 1), pl.ds(2 * c, 2)]
        return pltpu.make_async_copy(part, part, sem.at[c])

    def chunk_step(c, chunk_carry):
        all_of(in_ref, c, recv_sem).wait()
        vecs = jnp.concatenate(
            [in_ref[:, 2 * c + v].reshape(rows, 4 * W) for v in range(2)], axis=1
        )
        for p in range(2):
            zs_ref[p] = mm(vecs, tz_ref[p]).astype(bf)

        def y_step(i, carry):
            cols = []
            for k in range(2):
                at = pl.ds(pl.multiple_of((2 * i + k) * half, half), half)
                parts = [
                    zs_ref[p, at, d * lanes : (d + 1) * lanes] for p in range(2) for d in range(2)
                ]
                cols.append(jnp.concatenate(parts, axis=0))
            done = mm(ty_ref[...], jnp.concatenate(cols, axis=1))
            for k in range(2):
                for e in range(2):
                    start = pl.multiple_of((4 * i + 2 * k + e) * SPREAD, 8)
                    s_ref[pl.ds(start, G), :] = done[
                        e * G : (e + 1) * G, k * lanes : (k + 1) * lanes
                    ]
            return carry

        lax.fori_loop(0, W // 2, y_step, 0, unroll=4)

        def x_step(i, carry):
            first = 2 * X_GROUP * i
            ats = [pl.ds(first + k, 2 * W, stride=SPREAD) for k in range(2 * X_GROUP)]
            cols = [s_ref[at, :].astype(bf) for at in ats]
            for u in range(X_GROUP):
                done = mm(tx_ref[...], jnp.concatenate(cols[2 * u : 2 * u + 2], axis=1))
                real, imag = (done[:G], done[G:])
                pot = jnp.concatenate(
                    [pot_ref[first + 2 * u], pot_ref[first + 2 * u + 1]], axis=1
                )
                square = real * real + imag * imag
                for k in range(2):
                    dens_ref[first + 2 * u + k] += square[:, k * lanes : (k + 1) * lanes]
                weighted = jnp.concatenate(
                    [(real * pot).astype(bf), (imag * pot).astype(bf)], axis=0
                )
                back = mm(bx_ref[...], weighted)
                for k in range(2):
                    s_ref[ats[2 * u + k], :] = back[:, k * lanes : (k + 1) * lanes]
            return carry

        lax.fori_loop(0, G // (2 * X_GROUP), x_step, 0)

        def back_y_step(i, carry):
            cols = []
            for k in range(2):
                parts = []
                for e in range(2):
                    start = pl.multiple_of((4 * i + 2 * k + e) * SPREAD, 8)
                    parts.append(s_ref[pl.ds(start, G), :])
                cols.append(jnp.concatenate(parts, axis=0).astype(bf))
            done = mm(by_ref[...], jnp.concatenate(cols, axis=1)).astype(bf)
            for k in range(2):
                at = pl.ds(pl.multiple_of((2 * i + k) * half, half), half)
                for p in range(2):
                    for q in range(2):
                        r = (2 * p + q) * half
                        zs_ref[p, at, q * lanes : (q + 1) * lanes] = done[
                            r : r + half, k * lanes : (k + 1) * lanes
                        ]
            return carry

        lax.fori_loop(0, W // 2, back_y_step, 0, unroll=4)

        local = mm(zs_ref[0], bz_ref[0]) + mm(zs_ref[1], bz_ref[1])
        kin = kin_ref[...]
        npw_total = W * W * W
        for v in range(2):
            orb = in_ref[:, 2 * c + v].reshape(rows, 4 * W).astype(jnp.float32)
            ham = kin * orb + local[:, v * 4 * W : (v + 1) * 4 * W]
            numerator = jnp.sum(jnp.sum(orb * ham, axis=0, keepdims=True), axis=1, keepdims=True)
            denominator = jnp.sum(jnp.sum(orb * orb, axis=0, keepdims=True), axis=1, keepdims=True)
            ritz = numerator / npw_total / (denominator / npw_total + epsilon)
            search = ((ham - ritz * orb) / (1.0 + kin)).astype(bf)
            back_ref[:, 2 * c + v] = search.reshape(in_ref.shape[0], *in_ref.shape[2:])
            slot = lax.broadcasted_iota(jnp.int32, own_small_ref.shape, 1)
            here = slot == mine * orb_ref.shape[1] + 2 * c + v
            own_small_ref[...] = jnp.where(here, ritz, own_small_ref[...])
        at = pl.ds(2 * c, 2)
        search_ref[mine, at] = back_ref[mine, at]
        for k in range(1, count):
            peer = lax.rem(mine + k, count)
            pltpu.make_async_remote_copy(
                src_ref=back_ref.at[peer, at],
                dst_ref=search_ref.at[mine, at],
                send_sem=back_send_sem.at[c],
                recv_sem=back_recv_sem.at[c],
                device_id=device_of(peer, inner),
                device_id_type=MESH_ID,
            ).start()
        return chunk_carry

    lax.fori_loop(0, chunks, chunk_step, 0)

    outer = count // inner
    me_outer, me_inner = lax.axis_index(GROUP[0]), lax.axis_index(GROUP[1])
    bands, entries = c_ref.shape
    wide_lanes = 4 * W
    blocks = entries // wide_lanes
    per_inner = bands // inner
    each = orb_ref.shape[1] // HALVES
    vecs_half = BLOCK // HALVES
    two = 2 * vecs_half
    per_outer = two // outer
    spread = blocks + 8
    npw_total = W * W * W
    depth = entries // 4

    def remote(src, dst, send, recv, where):
        return pltpu.make_async_remote_copy(
            src_ref=src, dst_ref=dst, send_sem=send, recv_sem=recv,
            device_id=where, device_id_type=MESH_ID,
        )

    def to_inner(k):
        return lax.rem(me_inner + k, inner)

    def to_outer(k):
        return lax.rem(me_outer + k, outer)

    def rows_of(place):
        return pl.ds(pl.multiple_of(place * per_outer, per_outer), per_outer)

    def arrange(h):
        def wait_chunk(c, carry):
            all_of(search_ref, c, back_recv_sem).wait()
            return carry

        share = chunks // HALVES
        lax.fori_loop(h * share, (h + 1) * share, wait_chunk, 0)

        def widen(i, carry):
            for v in range(each):
                at = pl.ds(pl.multiple_of((i * each + v) * spread, 8), blocks)
                values = search_ref[i, h * each + v].reshape(blocks, wide_lanes)
                wide_ref[at, :] = values.astype(jnp.float32)
            return carry

        lax.fori_loop(0, count, widen, 0)

        def lay(j, carry):
            block = wide_ref[pl.ds(j, vecs_half, stride=spread), :]
            at = pl.ds(pl.multiple_of(j * wide_lanes, wide_lanes), wide_lanes)
            pair_ref[h, :vecs_half, at] = block.astype(bf)
            pair_ref[h, vecs_half:, at] = quarter_turn(block, 1.0).astype(bf)
            return carry

        lax.fori_loop(0, blocks, lay, 0)

    def overlap(h, quarter):
        rows = pl.ds(pl.multiple_of(quarter * per_inner, per_inner), per_inner)
        acc_ref[h] = jnp.zeros(acc_ref.shape[1:], jnp.float32)

        def step(i, carry):
            at = pl.ds(pl.multiple_of(i * depth, depth), depth)
            acc_ref[h] += lax.dot_general(
                pair_ref[h, :, at], c_ref[rows, at], (((1,), (1,)), ((), ())),
                preferred_element_type=jnp.float32,
            )
            return carry

        lax.fori_loop(0, entries // depth, step, 0)

    def first_copy(h, k):
        quarter, sem = to_inner(k), h * inner + k
        return remote(
            part_ref.at[h, quarter], got_ref.at[h, me_inner], send1.at[sem], recv1.at[sem],
            {GROUP[1]: quarter},
        )

    def overlap_all(h):
        def send_quarter(k, carry):
            quarter = to_inner(k)
            overlap(h, quarter)
            part_ref[h, quarter] = (acc_ref[h] / npw_total).astype(bf)
            first_copy(h, k).start()
            return carry

        lax.fori_loop(1, inner, send_quarter, 0)
        overlap(h, me_inner)

    def second_copy(h, k):
        place, sem = to_outer(k), h * outer + k
        return remote(
            mid_ref.at[h, rows_of(place)], got2_ref.at[h, me_outer], send2.at[sem], recv2.at[sem],
            {GROUP[0]: place},
        )

    def second_stage(h):
        total = acc_ref[h] / npw_total
        for k in range(1, inner):
            first_copy(h, k).wait_recv()
            total += got_ref[h, lax.rem(me_inner + inner - k, inner)].astype(jnp.float32)
        acc_ref[h] = total
        mid_ref[h] = total.astype(bf)
        for k in range(1, outer):
            second_copy(h, k).start()

    def z_copy(h, k):
        ref = all_ref.at[h, me_inner, rows_of(me_outer)]
        sem = h * outer + k
        return remote(ref, ref, send_z.at[sem], recv_z.at[sem], {GROUP[0]: to_outer(k)})

    def xy_copy(h, place, step, k):
        ref = all_ref.at[h, me_inner, rows_of(place)]
        sem = (h * outer + step) * inner + k
        return remote(ref, ref, send_xy.at[sem], recv_xy.at[sem], {GROUP[1]: to_inner(k)})

    def third_stage(h):
        total = acc_ref[h, rows_of(me_outer), :]
        for k in range(1, outer):
            second_copy(h, k).wait_recv()
            total += got2_ref[h, lax.rem(me_outer + outer - k, outer)].astype(jnp.float32)
        all_ref[h, me_inner, rows_of(me_outer), :] = total.astype(bf)
        for k in range(1, outer):
            z_copy(h, k).start()
        for k in range(1, inner):
            xy_copy(h, me_outer, 0, k).start()

    def forward(h):
        for step in range(1, outer):
            z_copy(h, step).wait_recv()
            place = lax.rem(me_outer + outer - step, outer)
            for k in range(1, inner):
                xy_copy(h, place, step, k).start()

    width = 4 * wide_lanes

    def project(h, quarter, first):
        rows = pl.ds(pl.multiple_of(quarter * per_inner, per_inner), per_inner)

        def step(i, carry):
            at = pl.ds(pl.multiple_of(i * width, width), width)
            done = mm(all_ref[h, quarter], c_ref[rows, at])
            proj_ref[h, :, at] = done if first else proj_ref[h, :, at] + done
            return carry

        lax.fori_loop(0, entries // width, step, 0)

    def project_rest(h):
        def rest(k, carry):
            for step in range(outer):
                xy_copy(h, me_outer, step, k).wait_recv()
            project(h, lax.rem(me_inner + inner - k, inner), False)
            return carry

        lax.fori_loop(1, inner, rest, 0)

    def small_copy(k):
        peer = lax.rem(mine + k, count)
        return remote(
            own_small_ref, smalls_ref.at[mine], send_s.at[k], recv_s.at[k], device_of(peer, inner)
        )

    def send_small(k, carry):
        small_copy(k).start()
        return carry

    load_c.wait()
    arrange(0)
    overlap_all(0)
    arrange(1)
    second_stage(0)
    overlap_all(1)
    third_stage(0)

    forces = partial_forces(dens_ref, pos_ref, strength_ref, gy_ref, gyd_ref, f_ref)
    for m in range(3):
        own_small_ref[m : m + 1, :] = forces[m]
    lax.fori_loop(1, count, send_small, 0)
    smalls_ref[mine] = own_small_ref[...]

    second_stage(1)
    forward(0)
    project(0, me_inner, True)
    third_stage(1)
    project_rest(0)
    forward(1)
    project(1, me_inner, True)

    for k in range(1, count):
        small_copy(k).wait_recv()
    summed = smalls_ref[0]
    for d in range(1, count):
        summed += smalls_ref[d]
    own = pos_ref[...]
    if images > 1:
        for side in range(2):
            near_copy(side).wait_recv()
        before = jnp.where(image == 0, start_ref[...], near_ref[0])
        after = jnp.where(image == images - 1, end_ref[...], near_ref[1])
    else:
        before, after = start_ref[...], end_ref[...]
    band, along = chain_forces(summed[:3], own, before, after)
    small_ref[...] = summed
    small_ref[:3] = band
    small_ref[4:5] = jnp.broadcast_to(along, (1, small_ref.shape[1]))

    project_rest(1)

    def close(j, carry):
        at = pl.ds(pl.multiple_of(j * wide_lanes, wide_lanes), wide_lanes)
        parts = []
        for h in range(HALVES):
            turned = quarter_turn(proj_ref[h, vecs_half:, at], -1.0)
            search = pair_ref[h, :vecs_half, at].astype(jnp.float32)
            left = search - (proj_ref[h, :vecs_half, at] + turned)
            parts.append(left.reshape(count, 1, each, wide_lanes))
        joined = jnp.concatenate(parts, axis=1).reshape(BLOCK, wide_lanes)
        out_ref[:, at] = joined.astype(bf)
        return carry

    lax.fori_loop(0, blocks, close, 0)

    def finish(c, carry):
        all_of(in_ref, c, send_sem).wait()
        all_of(search_ref, c, back_send_sem).wait()
        return carry

    lax.fori_loop(0, chunks, finish, 0)
    for k in range(1, count):
        small_copy(k).wait_send()
    for h in range(HALVES):
        for k in range(1, inner):
            first_copy(h, k).wait_send()
            for step in range(outer):
                xy_copy(h, me_outer, step, k).wait_send()
        for k in range(1, outer):
            second_copy(h, k).wait_send()
            z_copy(h, k).wait_send()
    if images > 1:
        for side in range(2):
            near_copy(side).wait_send()


def whole_step(flat_all, orbitals, own_pos, strength, start_pos, end_pos):
    devices, vectors, planes, half, lanes = orbitals.shape
    inner, outer = lax.axis_size(GROUP[1]), lax.axis_size(GROUP[0])
    bands, entries = flat_all.shape
    atoms = own_pos.shape[1]
    tabs = kernel_tables()
    kin = jnp.asarray(kinetic_table())
    whole = pl.BlockSpec(memory_space=pltpu.VMEM)
    chunks = vectors // 2
    f32, bf = jnp.float32, jnp.bfloat16
    sem, vmem = pltpu.SemaphoreType.DMA, pltpu.VMEM
    two = 2 * BLOCK // HALVES
    share = bands // inner
    flops = vectors * 2 * 2 * (W * W * 2 * W * 2 * G + W * G * 2 * W * 2 * G + G * G * 2 * W * 2 * G)
    flops += 8 * BLOCK * bands * entries
    return pl.pallas_call(
        step_kernel,
        in_specs=[pl.BlockSpec(memory_space=pltpu.HBM)] + [whole] * 12,
        out_specs=[whole] * 2,
        out_shape=[
            jax.ShapeDtypeStruct((BLOCK, entries), bf),
            jax.ShapeDtypeStruct((8, atoms), f32),
        ],
        scratch_shapes=[
            vmem((bands, entries), bf),
            vmem(orbitals.shape, bf),
            vmem(orbitals.shape, bf),
            vmem(orbitals.shape, bf),
            vmem((2, W * W // 2, 4 * G), bf),
            vmem((2 * W * SPREAD, 2 * G), f32),
            vmem((G, G, 2 * G), f32),
            vmem((G, G, 2 * G), f32),
            vmem((G, atoms), f32),
            vmem((G, atoms), f32),
            vmem((3, G, atoms), f32),
            vmem((BLOCK // HALVES * (entries // (4 * W) + 8), 4 * W), f32),
            vmem((HALVES, two, entries), bf),
            vmem((HALVES, inner, two, share), bf),
            vmem((HALVES, inner, two, share), bf),
            vmem((HALVES, two, share), bf),
            vmem((HALVES, outer, two // outer, share), bf),
            vmem((HALVES, inner, two, share), bf),
            vmem((HALVES, two, entries), f32),
            vmem((HALVES, two, share), f32),
            vmem((8, atoms), f32),
            vmem((devices, 8, atoms), f32),
            vmem((2, 3, atoms), jnp.int32),
            sem((1,)), sem((chunks,)), sem((chunks,)), sem((chunks,)), sem((chunks,)),
            sem((HALVES * inner,)), sem((HALVES * inner,)),
            sem((HALVES * outer,)), sem((HALVES * outer,)),
            sem((HALVES * outer,)), sem((HALVES * outer,)),
            sem((HALVES * inner * outer,)), sem((HALVES * inner * outer,)),
            sem((devices,)), sem((devices,)), sem((2,)), sem((2,)),
        ],
        compiler_params=pltpu.CompilerParams(
            collective_id=0, has_side_effects=True, vmem_limit_bytes=48 * 1024 * 1024
        ),
        cost_estimate=pl.CostEstimate(flops=flops, bytes_accessed=16 << 20, transcendentals=0),
        name="whole_step",
    )(flat_all, orbitals, own_pos, strength, start_pos, end_pos, kin, *tabs)


def body(coefficients, rotation, positions, start_pos, end_pos, species, depth):
    devices = lax.axis_size(GROUP)
    coeff_all = coefficients[0]
    planes = coeff_all.shape[1]
    flat_all = coeff_all.reshape(BANDS, -1)
    vectors = BLOCK // devices
    orbitals = jnp.einsum("ib,ik->bk", rotation[0], flat_all, preferred_element_type=jnp.float32)
    orbitals = orbitals.astype(jnp.bfloat16)
    orbitals = orbitals.reshape(devices, vectors, planes, W // 2, 4 * W)
    kind_ids = jnp.arange(SPECIES, dtype=jnp.int32)
    strength = jnp.sum(jnp.where(species[:, None] == kind_ids[None, :], depth[None, :], 0.0), 1)
    strength = strength[None]
    own_pos = positions[0]
    correction, small = whole_step(flat_all, orbitals, own_pos, strength, start_pos, end_pos)
    correction = correction.reshape(BLOCK, planes, W * 2 * W)
    return (correction[None], small[3:4], small[None, :3], small[4, :1])


def solution(mesh):
    in_specs = (
        P("img", None, ("band", "pw"), None),
        P("img", None, None),
        P("img", None, None),
        P(),
        P(),
        P(),
        P(),
    )
    out_specs = (
        P("img", None, ("band", "pw"), None),
        P("img", None),
        P("img", None, None),
        P("img"),
    )
    return jax.shard_map(body, mesh=mesh, in_specs=in_specs, out_specs=out_specs, check_vma=False)
```
